32 devices in a mesh: tok: 4 (over y, x), hid: 2 (over core), voc: 4 (over z).
Axes of the slice: x: 2, y: 2, z: 4, core: 2. Of those that a mesh axis runs over, the one named last changes fastest.
Arguments:
- student_hidden: bfloat16 [512, 8192], P('tok', ('hid', 'voc')), may hold values from -8 to 8
- teacher_hidden: bfloat16 [512, 16384], P('tok', ('hid', 'voc')), may hold values from -8 to 8
- student_head: bfloat16 [8192, 2048], P('hid', 'voc'), may hold values from -2 to 2
- teacher_head: bfloat16 [16384, 2048], P('hid', 'voc'), may hold values from -2 to 2
- loss_weight: float32 [512], P('tok'), may hold values from 128 to 1024
Outputs:
- grad_hidden: bfloat16 [512, 8192], P('tok', ('hid', 'voc'))
- mean_loss: float32 [], replicated
The draws below stay inside these ranges and needn't reach their ends.
All inputs are finite; a program needn't handle non-finite values.
Results may differ from the reference program's by a relative error of at most 0.001.
The reference program's roundings to bfloat16 on the way (of `scaled_gap`) count: a program that leaves them out, or rounds other values in their place, can miss the bound.
Values may be sent and summed in bfloat16 or wider, within the bound.
A program may use at most 64 MiB of HBM per device.

```python
import math
import jax
import jax.numpy as jnp

DS = 8192
DT = 16384
TOKENS = 512
V = 2048


def head_values(key, width, salt):
    values = jax.random.normal(jax.random.fold_in(key, salt), (width, V), jnp.float32)
    return jnp.clip(values, -5.0, 5.0) * (2.0 / math.sqrt(width))


def hidden_values(key, width, head_salt, salt):
    values = jnp.clip(jax.random.normal(jax.random.fold_in(key, salt), (TOKENS, width), jnp.float32), -6.0, 6.0)
    return values


def draw_student_head(key, part):
    return head_values(key, DS, 11).astype(jnp.bfloat16)


def draw_teacher_head(key, part):
    return head_values(key, DT, 12).astype(jnp.bfloat16)


def draw_student_hidden(key, part):
    return hidden_values(key, DS, 11, 13).astype(jnp.bfloat16)


def draw_teacher_hidden(key, part):
    return hidden_values(key, DT, 12, 14).astype(jnp.bfloat16)


def block_levels(stream_key, shape, pieces, least, high):
    level = 1.0
    for dim, blocks in pieces:
        steps = jax.random.uniform(jax.random.fold_in(jax.random.fold_in(stream_key, 6), dim), (blocks,), jnp.float32, least / len(pieces), high / len(pieces))
        level = level * jnp.repeat(jnp.exp(steps), shape[dim] // blocks).reshape((-1,) + (1,) * (len(shape) - 1 - dim))
    return level


def setup_inputs(seed: int = 0) -> dict:
    key_of = jax.random.split(jax.random.key(seed), 6)
    return {
        "student_hidden": draw_student_hidden(jax.random.fold_in(key_of[5], 71), 0),
        "teacher_hidden": draw_teacher_hidden(jax.random.fold_in(key_of[5], 71), 0),
        "student_head": draw_student_head(jax.random.fold_in(key_of[5], 71), 0),
        "teacher_head": draw_teacher_head(jax.random.fold_in(key_of[5], 71), 0),
        "loss_weight": jnp.clip(jnp.exp(math.log(1024.0) - 2.0794415 * jax.random.uniform(key_of[4], (TOKENS,), jnp.float32) ** block_levels(key_of[4], (TOKENS,), ((0, 4),), -0.2, 0.2)), 128.0, 1024.0),
    }


def reference(student_hidden, teacher_hidden, student_head, teacher_head, loss_weight):
    student_logits = jnp.dot(student_hidden, student_head, preferred_element_type=jnp.float32)
    teacher_logits = jnp.dot(teacher_hidden, teacher_head, preferred_element_type=jnp.float32)
    student_peak = jnp.max(student_logits, axis=1)
    teacher_peak = jnp.max(teacher_logits, axis=1)
    student_lse = student_peak + jnp.log(jnp.sum(jnp.exp(student_logits - student_peak[:, None]), axis=1))
    teacher_lse = teacher_peak + jnp.log(jnp.sum(jnp.exp(teacher_logits - teacher_peak[:, None]), axis=1))
    teacher_prob = jnp.exp(teacher_logits - teacher_lse[:, None])
    student_prob = jnp.exp(student_logits - student_lse[:, None])
    divergence = jnp.sum(teacher_prob * (teacher_logits - student_logits), axis=1) - teacher_lse + student_lse
    mean_loss = jnp.sum(divergence) / TOKENS
    scaled_gap = (loss_weight[:, None] * (student_prob - teacher_prob)).astype(jnp.bfloat16)
    grad_hidden = jax.lax.dot_general(scaled_gap, student_head, (((1,), (1,)), ((), ())), preferred_element_type=jnp.float32)
    return grad_hidden.astype(jnp.bfloat16), mean_loss
```

```python
import functools

import jax
import jax.numpy as jnp
from jax import lax
from jax.experimental import pallas as pl
from jax.experimental.pallas import tpu as pltpu
from jax.sharding import PartitionSpec as P

MESH = pl.DeviceIdType.MESH
F32 = jnp.float32
BF16 = jnp.bfloat16
GROUPS = 2


def fused(n, nt, ng, x_hbm, y_hbm, w_hbm, sw_hbm, tw_hbm, out, loss_out,
          x_ref, y_ref, w_ref, wf, tw, tg, sp, spx, ssum, srr, tacc, tpx, stat, gap, wcol, lossb, lossr, lossx, acc,
          lc, wz_s, wz_r, wt_s, wt_r, th_s, th_r, px_s, px_r, tx_s, tx_r, rs_s, rs_r,
          st_s, st_r, gz_s, gz_r, gx_s, gx_r, ls_s, ls_r):
    z = lax.axis_index("voc")
    t = lax.axis_index("tok")
    h = lax.axis_index("hid")
    rows, ks = x_ref.shape
    kt = y_ref.shape[1]
    half = rows // 2
    q = half // ng
    quarter = ks // nt
    eighth = quarter // 2
    partner = {"hid": 1 - h}
    mine = pl.ds(pl.multiple_of(h * half, half), half)
    theirs = pl.ds(pl.multiple_of((1 - h) * half, half), half)
    nbr = (t + 1 - 2 * lax.rem(t, 2), lax.rem(t + 2, 4))
    diag = nt - 1 - t
    at_end = jnp.logical_or(z == 0, z == n - 1)
    inside = jnp.logical_not(at_end)
    side_in = jnp.where(z < n // 2, 1, 0)
    side_out = 1 - side_in
    step_in = 2 * side_in - 1
    near, mid, far = z + step_in, z + 2 * step_in, z + 3 * step_in
    inner, beyond, outer = z + step_in, z + 2 * step_in, z - step_in

    def rc(src, dst, ss, rs, dev):
        return pltpu.make_async_remote_copy(
            src_ref=src, dst_ref=dst, send_sem=ss, recv_sem=rs,
            device_id=dev, device_id_type=MESH)

    def zdev(k):
        return lax.rem(z + k, n)

    def group(c, g):
        return pl.ds(pl.multiple_of(c * half + g * q, q), q)

    own_w = pltpu.make_async_copy(sw_hbm.at[pl.ds(pl.multiple_of(z * ks, ks), ks)], wf.at[z], lc.at[n])
    own_w.start()
    ins = [pltpu.make_async_copy(a, b, lc.at[n + 1 + i])
           for i, (a, b) in enumerate(((x_hbm, x_ref), (y_hbm, y_ref), (w_hbm, w_ref)))]
    for c in ins:
        c.start()

    def tw_copy(i):
        return pltpu.make_async_copy(tw_hbm.at[pl.ds(pl.multiple_of(i * kt, kt), kt)], tw.at[i], lc.at[i])

    barrier = pltpu.get_barrier_semaphore()
    for k in range(1, n):
        pl.semaphore_signal(barrier, inc=1, device_id={"voc": zdev(k)}, device_id_type=MESH)
    for k in range(1, nt):
        pl.semaphore_signal(barrier, inc=1, device_id={"tok": lax.rem(t + k, nt)}, device_id_type=MESH)
    pl.semaphore_signal(barrier, inc=1, device_id=partner, device_id_type=MESH)
    pl.semaphore_wait(barrier, n - 1 + nt - 1 + 1)

    def part(i):
        return pl.ds(pl.multiple_of(i * quarter, quarter), quarter)

    def subpart(i, b):
        return pl.ds(pl.multiple_of(i * quarter + b * eighth, eighth), eighth)

    def wz(j):
        return rc(sw_hbm.at[pl.ds(pl.multiple_of(j * ks + t * quarter, quarter), quarter)],
                  wf.at[z, part(t)], wz_s.at[j], wz_r.at[z], {"voc": j})

    def wz_in(j):
        return rc(wf.at[j, part(t)], wf.at[j, part(t)], wz_s.at[j], wz_r.at[j], {"voc": j})

    def wt(j, k):
        return rc(wf.at[j, part(t)], wf.at[j, part(t)], wt_s.at[j, k], wt_r.at[j, k], {"tok": nbr[k]})

    def wt_in(j, k):
        return rc(wf.at[j, part(nbr[k])], wf.at[j, part(nbr[k])], wt_s.at[j, k], wt_r.at[j, k], {"tok": nbr[k]})

    def wd(j, k):
        piece = wf.at[j, subpart(nbr[k], k)]
        return rc(piece, piece, wt_s.at[j, 2 + k], wt_r.at[j, 2 + k], {"tok": nbr[1 - k]})

    def wd_in(j, k):
        piece = wf.at[j, subpart(diag, k)]
        return rc(piece, piece, wt_s.at[j, 2 + k], wt_r.at[j, 2 + k], {"tok": nbr[1 - k]})

    def y_send(src, i, g, c, k, dev):
        return rc(src.at[group(c, g)], tg.at[i, group(c, g)], th_s.at[k, 2 * g + c], th_r.at[i, 2 * g + c], {"voc": dev})

    def y_own(g, c, k, dev):
        return y_send(y_hbm, z, g, c, k, dev)

    def y_relay(i, g, c, k):
        return y_send(tg.at[i], i, g, c, k, outer)

    def y_out(g, k, dev, cs=(0, 1)):
        for c in cs:
            y_own(g, c, k, dev).start()

    @pl.when(at_end)
    def _():
        for j in (near, mid, far):
            wz(j).start()
        y_out(0, 0, near)

    @pl.when(inside)
    def _():
        for j in (outer, inner, beyond):
            wz(j).start()
        y_out(0, 1, outer)
        y_out(0, 0, inner)
        for g in range(1, ng):
            y_out(g, 1, outer)
            y_out(g, 0, inner)

    for k in range(n):
        tw_copy(zdev(k)).start()

    for c in ins:
        c.wait()
    wcol[...] = jnp.transpose(jnp.broadcast_to(w_ref[...], (rows, rows)))

    def w_arrive(j):
        wz_in(j).wait_recv()
        for k in range(2):
            wt(j, k).start()

    def w_spread(j):
        for k in range(2):
            wt_in(j, k).wait_recv()
            wd(j, k).start()

    def teacher_dot(src, i, g, first):
        step = kt // 2

        @pl.loop(0, 2)
        def _(s):
            cols = pl.ds(pl.multiple_of(s * step, step), step)
            both = jnp.concatenate([src[pl.ds(c * half + g * q, q), cols] for c in range(2)], axis=0)
            term = jnp.dot(both, tw[i, cols, :], preferred_element_type=F32)
            if first:
                @pl.when(s == 0)
                def _():
                    tacc[g] = term

                @pl.when(s > 0)
                def _():
                    tacc[g] += term
            else:
                tacc[g] += term

    def take_y(i, g, c, k=None):
        y_send(tg.at[i], i, g, c, 0, outer).wait_recv()
        if k is not None:
            y_relay(i, g, c, k).start()

    def dot_y(i, g):
        teacher_dot(tg.at[i], i, g, False)

    def full_y(i, g, k=None):
        for c in range(2):
            take_y(i, g, c, k)
        dot_y(i, g)

    def student(j):
        sp[j] = jnp.dot(x_ref[...], wf[j], preferred_element_type=F32)
        rc(sp.at[j, theirs], spx.at[j], px_s.at[j], px_r.at[j], partner).start()

    def student_sum(j):
        rc(sp.at[j, theirs], spx.at[j], px_s.at[j], px_r.at[j], partner).wait_recv()
        ssum[j] = sp[j, mine, :] + spx[j]

    def rs(side, j):
        return rc(ssum.at[j], srr.at[side, j], rs_s.at[j], rs_r.at[side, j], {"voc": z + 2 * side - 1})

    def student_full(j):
        for k in range(2):
            wd_in(j, k).wait_recv()
        student(j)

    def rs_take(side, j):
        rs(side, j).wait_recv()
        ssum[j] += srr[side, j]

    def student_pass(j, side, upstream):
        student_sum(j)
        if upstream:
            rs_take(side, j)
        rs(side, j).start()

    def t_swap(g):
        return rc(tacc.at[g, pl.ds(pl.multiple_of((1 - h) * q, q), q)], tpx.at[g], tx_s.at[g], tx_r.at[g], partner)

    def stx(g, j, src):
        return rc(stat.at[g, src], stat.at[g, src], st_s.at[g, j], st_r.at[g, src], {"voc": j})

    def gz(g, j, src):
        return rc(gap.at[src, group(h, g)], gap.at[src, group(h, g)], gz_s.at[g, j], gz_r.at[g, src], {"voc": j})

    def gx(g, src, c):
        return rc(gap.at[src, group(c, g)], gap.at[src, group(c, g)], gx_s.at[g, src], gx_r.at[g, src], partner)

    def send_stats(g):
        t_swap(g).wait_recv()
        tl = tacc[g, pl.ds(pl.multiple_of(h * q, q), q), :] + tpx[g]
        tpx[g] = tl
        sl = ssum[z, pl.ds(g * q, q), :]
        ms = jnp.max(sl, axis=1, keepdims=True)
        ss = jnp.sum(jnp.exp(sl - ms), axis=1, keepdims=True)
        mt = jnp.max(tl, axis=1, keepdims=True)
        et = jnp.exp(tl - mt)
        st = jnp.sum(et, axis=1, keepdims=True)
        cr = jnp.sum(et * (tl - sl), axis=1, keepdims=True)
        lane = lax.broadcasted_iota(jnp.int32, (q, 128), 1)
        cols = jnp.where(lane == 0, ms, jnp.where(lane == 1, mt, jnp.where(
            lane == 2, ss, jnp.where(lane == 3, st, cr))))
        stat[g, z] = jnp.transpose(jnp.concatenate([cols] * (128 // q), axis=0))[:8]
        for k in (2, 1, 3):
            stx(g, zdev(k), z).start()

    def send_gap(g):
        for k in range(1, n):
            stx(g, zdev(k), zdev(k)).wait_recv()
        parts = [stat[g, j] for j in range(n)]
        top = parts[0]
        for p in parts[1:]:
            top = jnp.maximum(top, p)
        big_s, big_t = top[0:1], top[1:2]
        tot_s = jnp.zeros_like(big_s)
        tot_t = jnp.zeros_like(big_s)
        cross = jnp.zeros_like(big_s)
        for p in parts:
            es = jnp.exp(p[0:1] - big_s)
            ets = jnp.exp(p[1:2] - big_t)
            tot_s = tot_s + p[2:3] * es
            tot_t = tot_t + p[3:4] * ets
            cross = cross + p[4:5] * ets
        lse_s = big_s + jnp.log(tot_s)
        lse_t = big_t + jnp.log(tot_t)
        scale = wcol[group(h, g), :][:, 0:1]
        sub = lax.broadcasted_iota(jnp.int32, (128, 128), 0)
        back = jnp.transpose(jnp.where(sub == 0, lse_s, lse_t))[:q]
        col_s, col_t = back[:, 0:1], back[:, 1:2]
        sl = ssum[z, pl.ds(g * q, q), :]
        gap[z, group(h, g), :] = (scale * (jnp.exp(sl - col_s) - jnp.exp(tpx[g] - col_t))).astype(BF16)
        for k in (2, 1, 3):
            gz(g, zdev(k), z).start()
        gx(g, z, h).start()
        div = cross / tot_t - lse_t + lse_s
        first = lax.broadcasted_iota(jnp.int32, div.shape, 1) < q
        lossr[g] = jnp.broadcast_to(jnp.sum(jnp.where(first, div, 0.0), axis=1, keepdims=True), (8, 128))

    def take_gap(g, j):
        gz(g, j, j).wait_recv()
        gx(g, j, h).start()

    def grad_dot(g, j, first):
        gx(g, j, 1 - h).wait_recv()
        both = jnp.concatenate([gap[j, pl.ds(c * half + g * q, q), :] for c in range(2)], axis=0)
        term = lax.dot_general(both, wf[j], (((1,), (1,)), ((), ())), preferred_element_type=F32)
        if first:
            acc[g] = term
        else:
            acc[g] += term

    def store(g):
        for c in range(2):
            out[pl.ds(c * half + g * q, q), :] = acc[g, pl.ds(c * q, q), :].astype(BF16)

    def local_dots():
        for i in range(n):
            tw_copy(i).wait()
        for g in range(ng):
            teacher_dot(y_ref, z, g, True)
        own_w.wait()
        student(z)

    @pl.when(at_end)
    def _():
        w_arrive(near)
        local_dots()
        w_spread(near)
        student_full(near)
        w_arrive(far)
        w_spread(far)
        y_out(0, 1, mid)
        student_pass(near, side_in, False)
        w_arrive(mid)
        student_full(far)
        full_y(near, 0)
        student_pass(far, side_in, False)
        w_spread(mid)
        full_y(near, 1)
        student_full(mid)

        @pl.when(h == 1)
        def _():
            y_out(1, 1, mid)
        student_sum(z)
        student_pass(mid, side_in, False)

        @pl.when(h == 0)
        def _():
            y_out(1, 1, mid)
        y_out(1, 0, near)
        full_y(far, 0)
        full_y(mid, 0)
        t_swap(0).start()
        full_y(mid, 1)
        rs_take(side_out, z)
        send_stats(0)
        full_y(far, 1)
        t_swap(1).start()

    @pl.when(inside)
    def _():
        w_arrive(outer)
        local_dots()
        w_spread(outer)
        w_arrive(inner)
        w_arrive(beyond)
        student_full(outer)
        w_spread(inner)
        w_spread(beyond)
        take_y(inner, 0, 0, 3)
        take_y(beyond, 0, 0, 2)
        student_full(inner)
        take_y(inner, 0, 1, 3)
        take_y(beyond, 0, 1, 2)
        full_y(outer, 0)
        student_full(beyond)
        dot_y(beyond, 0)
        student_pass(beyond, side_in, True)
        dot_y(inner, 0)
        t_swap(0).start()
        take_y(inner, 1, 0, 3)
        take_y(inner, 1, 1, 3)
        student_pass(outer, side_out, True)
        dot_y(inner, 1)
        take_y(beyond, 1, 0, 2)
        take_y(beyond, 1, 1, 2)
        student_pass(inner, side_in, True)
        dot_y(beyond, 1)
        student_sum(z)
        rs_take(side_in, z)
        rs_take(side_out, z)
        send_stats(0)
        full_y(outer, 1)
        t_swap(1).start()

    def lp():
        return rc(lossb.at[0], lossb.at[1], ls_s.at[nt], ls_r.at[nt], partner)

    def ls(a, b):
        return rc(lossx.at[b], lossx.at[b], ls_s.at[a], ls_r.at[b], {"tok": a})

    send_stats(1)
    send_gap(0)
    send_gap(1)
    lossb[0] = lossr[0] + lossr[1]
    lp().start()
    across = lax.rem(z + 2, n)
    order = (near, across, n * (n - 1) // 2 - z - near - across)
    grad_dot(0, z, True)
    for j in order:
        take_gap(0, j)
    lp().wait_recv()
    lossx[t] = lossb[0] + lossb[1]
    for k in range(1, nt):
        ls(lax.rem(t + k, nt), t).start()
    grad_dot(1, z, True)
    for j in order:
        grad_dot(0, j, False)
    store(0)
    for j in order:
        take_gap(1, j)
    for j in order:
        grad_dot(1, j, False)
    store(1)
    for k in range(1, nt):
        ls(t, lax.rem(t + k, nt)).wait_recv()
    total = lossx[0]
    for a in range(1, nt):
        total = total + lossx[a]
    loss_out[0, 0] = total[0, 0] / (rows * nt)

    for k in range(1, n):
        j = zdev(k)
        wz(j).wait_send()
        for b in range(2):
            wt(j, b).wait_send()
            wd(j, b).wait_send()
        rs(side_in, j).wait_send()
    for g in range(ng):
        for k in range(1, n):
            stx(g, zdev(k), z).wait_send()
            gz(g, zdev(k), z).wait_send()
        for c in range(2):
            y_own(g, c, 0, near).wait_send()

            @pl.when(at_end)
            def _(g=g, c=c):
                y_own(g, c, 1, mid).wait_send()

            @pl.when(inside)
            def _(g=g, c=c):
                y_own(g, c, 1, outer).wait_send()
                for k, j in ((2, beyond), (3, inner)):
                    y_relay(j, g, c, k).wait_send()
        for j in range(n):
            gx(g, j, h).wait_send()
        t_swap(g).wait_send()
    for j in range(n):
        rc(sp.at[j, theirs], spx.at[j], px_s.at[j], px_r.at[j], partner).wait_send()
    lp().wait_send()
    for k in range(1, nt):
        ls(lax.rem(t + k, nt), t).wait_send()


def fused_shards(n, nt, student_hidden, teacher_hidden, student_head, teacher_head, loss_weight):
    rows, ks = student_hidden.shape
    kt = teacher_hidden.shape[1]
    v = student_head.shape[1]
    half = rows // 2
    ng = GROUPS
    q = half // ng
    dma = lambda *s: pltpu.SemaphoreType.DMA(s)
    vmem = lambda s, d: pltpu.VMEM(s, d)
    whole = pl.BlockSpec(memory_space=pltpu.VMEM)
    anywhere = pl.BlockSpec(memory_space=pl.ANY)
    grad, loss = pl.pallas_call(
        functools.partial(fused, n, nt, ng),
        out_shape=(jax.ShapeDtypeStruct((rows, ks), BF16), jax.ShapeDtypeStruct((1, 1), F32)),
        in_specs=[anywhere] * 5,
        out_specs=(whole, pl.BlockSpec(memory_space=pltpu.SMEM)),
        scratch_shapes=[
            vmem((rows, ks), BF16),
            vmem((rows, kt), BF16),
            vmem((1, rows), F32),
            vmem((n, ks, v), BF16),
            vmem((n, kt, v), BF16),
            vmem((n, rows, kt), BF16),
            vmem((n, rows, v), F32),
            vmem((n, half, v), F32),
            vmem((n, half, v), F32),
            vmem((2, n, half, v), F32),
            vmem((ng, 2 * q, v), F32),
            vmem((ng, q, v), F32),
            vmem((ng, n, 8, 128), F32),
            vmem((n, rows, v), BF16),
            vmem((rows, rows), F32),
            vmem((2, 8, 128), F32),
            vmem((ng, 8, 128), F32),
            vmem((nt, 8, 128), F32),
            vmem((ng, 2 * q, ks), F32),
            dma(n + 4),
            dma(n), dma(n), dma(n, 4), dma(n, 4),
            dma(4, 2 * ng), dma(n, 2 * ng),
            dma(n), dma(n), dma(ng), dma(ng), dma(n), dma(2, n),
            dma(ng, n), dma(ng, n), dma(ng, n), dma(ng, n), dma(ng, n), dma(ng, n),
            dma(nt + 1), dma(nt + 1),
        ],
        compiler_params=pltpu.CompilerParams(
            collective_id=0, has_side_effects=True, vmem_limit_bytes=60 << 20),
        name="divergence_grad",
    )(student_hidden, teacher_hidden, loss_weight.reshape(1, rows), student_head, teacher_head)
    return grad, loss.reshape(())


def divergence_terms(student_logits, teacher_logits, weights):
    differences = teacher_logits - student_logits
    peak_student, peak_teacher = lax.pmax(
        (jnp.max(student_logits, axis=1), jnp.max(teacher_logits, axis=1)), "voc"
    )
    scaled_student = jnp.exp(student_logits - peak_student[:, None])
    scaled_teacher = jnp.exp(teacher_logits - peak_teacher[:, None])
    total_student, total_teacher, cross_sum = lax.psum(
        (
            jnp.sum(scaled_student, axis=1),
            jnp.sum(scaled_teacher, axis=1),
            jnp.sum(scaled_teacher * differences, axis=1),
        ),
        "voc",
    )
    student_lse = peak_student + jnp.log(total_student)
    teacher_lse = peak_teacher + jnp.log(total_teacher)
    divergence = cross_sum / total_teacher - teacher_lse + student_lse
    prob_gap = jnp.exp(student_logits - student_lse[:, None]) - jnp.exp(
        teacher_logits - teacher_lse[:, None]
    )
    scaled_gap = (weights[:, None] * prob_gap).astype(jnp.bfloat16)
    return (divergence, scaled_gap)


def plain_shards(student_hidden, teacher_hidden, student_head, teacher_head, loss_weight):
    student_block, teacher_block = (
        lax.all_gather(student_hidden, "voc", axis=1, tiled=True),
        lax.all_gather(teacher_hidden, "voc", axis=1, tiled=True),
    )
    vocab_local = student_head.shape[1]
    row_count = student_block.shape[0] // lax.axis_size("hid")
    joined = lax.psum_scatter(
        jnp.concatenate(
            [
                jnp.dot(student_block, student_head, preferred_element_type=jnp.float32),
                jnp.dot(teacher_block, teacher_head, preferred_element_type=jnp.float32),
            ],
            axis=1,
        ),
        "hid",
        scatter_dimension=0,
        tiled=True,
    )
    student_logits = joined[:, :vocab_local]
    teacher_logits = joined[:, vocab_local:]
    weights = lax.dynamic_slice_in_dim(loss_weight, lax.axis_index("hid") * row_count, row_count)
    divergence, scaled_gap = divergence_terms(student_logits, teacher_logits, weights)
    token_total = loss_weight.shape[0] * lax.axis_size("tok")
    loss_total = lax.psum(jnp.sum(divergence), ("tok", "hid"))
    grad_terms = lax.dot_general(
        lax.all_gather(scaled_gap, "hid", axis=0, tiled=True),
        student_head,
        (((1,), (1,)), ((), ())),
        preferred_element_type=jnp.float32,
    )
    grad_hidden = lax.psum_scatter(grad_terms, "voc", scatter_dimension=1, tiled=True).astype(
        jnp.bfloat16
    )
    mean_loss = loss_total / token_total
    return (grad_hidden, mean_loss)


def solution(mesh):
    placed = (
        P("tok", ("hid", "voc")),
        P("tok", ("hid", "voc")),
        P("hid", "voc"),
        P("hid", "voc"),
        P("tok"),
    )
    n, nt = mesh.shape["voc"], mesh.shape["tok"]
    if n == 4 and nt == 4 and mesh.shape["hid"] == 2:
        body = functools.partial(fused_shards, n, nt)
    else:
        body = plain_shards
    return jax.shard_map(
        body,
        mesh=mesh,
        in_specs=placed,
        out_specs=(P("tok", ("hid", "voc")), P()),
        check_vma=False,
    )
```

```python
import functools

import jax
import jax.numpy as jnp
from jax import lax
from jax.experimental import pallas as pl
from jax.experimental.pallas import tpu as pltpu
from jax.sharding import PartitionSpec as P

MESH = pl.DeviceIdType.MESH
F32 = jnp.float32
BF16 = jnp.bfloat16
GROUPS = 2


def fused(n, nt, ng, x_hbm, y_hbm, w_hbm, sw_hbm, tw_hbm, out, loss_out,
          x_ref, y_ref, w_ref, wf, tw, tg, sp, spx, ssum, srr, tacc, tpx, stat, gap, wcol, lossb, lossr, lossx, acc, stage,
          lc, wz_s, wz_r, wt_s, wt_r, th_s, th_r, px_s, px_r, tx_s, tx_r, rs_s, rs_r,
          st_s, st_r, gz_s, gz_r, gx_s, gx_r, ls_s, ls_r, oc):
    z = lax.axis_index("voc")
    t = lax.axis_index("tok")
    h = lax.axis_index("hid")
    rows, ks = x_ref.shape
    kt = y_ref.shape[1]
    half = rows // 2
    q = half // ng
    quarter = ks // nt
    eighth = quarter // 2
    partner = {"hid": 1 - h}
    mine = pl.ds(pl.multiple_of(h * half, half), half)
    theirs = pl.ds(pl.multiple_of((1 - h) * half, half), half)
    nbr = (t + 1 - 2 * lax.rem(t, 2), lax.rem(t + 2, 4))
    diag = nt - 1 - t
    at_end = jnp.logical_or(z == 0, z == n - 1)
    inside = jnp.logical_not(at_end)
    side_in = jnp.where(z < n // 2, 1, 0)
    side_out = 1 - side_in
    step_in = 2 * side_in - 1
    near, mid, far = z + step_in, z + 2 * step_in, z + 3 * step_in
    inner, beyond, outer = z + step_in, z + 2 * step_in, z - step_in

    def rc(src, dst, ss, rs, dev):
        return pltpu.make_async_remote_copy(
            src_ref=src, dst_ref=dst, send_sem=ss, recv_sem=rs,
            device_id=dev, device_id_type=MESH)

    def zdev(k):
        return lax.rem(z + k, n)

    def group(c, g):
        return pl.ds(pl.multiple_of(c * half + g * q, q), q)

    own_w = pltpu.make_async_copy(sw_hbm.at[pl.ds(pl.multiple_of(z * ks, ks), ks)], wf.at[z], lc.at[n])
    own_w.start()
    ins = [pltpu.make_async_copy(a, b, lc.at[n + 1 + i])
           for i, (a, b) in enumerate(((x_hbm, x_ref), (y_hbm, y_ref), (w_hbm, w_ref)))]
    for c in ins:
        c.start()

    def tw_copy(i):
        return pltpu.make_async_copy(tw_hbm.at[pl.ds(pl.multiple_of(i * kt, kt), kt)], tw.at[i], lc.at[i])

    barrier = pltpu.get_barrier_semaphore()
    for k in range(1, n):
        pl.semaphore_signal(barrier, inc=1, device_id={"voc": zdev(k)}, device_id_type=MESH)
    for k in range(1, nt):
        pl.semaphore_signal(barrier, inc=1, device_id={"tok": lax.rem(t + k, nt)}, device_id_type=MESH)
    pl.semaphore_signal(barrier, inc=1, device_id=partner, device_id_type=MESH)
    pl.semaphore_wait(barrier, n - 1 + nt - 1 + 1)

    def part(i):
        return pl.ds(pl.multiple_of(i * quarter, quarter), quarter)

    def subpart(i, b):
        return pl.ds(pl.multiple_of(i * quarter + b * eighth, eighth), eighth)

    def wz(j):
        return rc(sw_hbm.at[pl.ds(pl.multiple_of(j * ks + t * quarter, quarter), quarter)],
                  wf.at[z, part(t)], wz_s.at[j], wz_r.at[z], {"voc": j})

    def wz_in(j):
        return rc(wf.at[j, part(t)], wf.at[j, part(t)], wz_s.at[j], wz_r.at[j], {"voc": j})

    def wt(j, k):
        return rc(wf.at[j, part(t)], wf.at[j, part(t)], wt_s.at[j, k], wt_r.at[j, k], {"tok": nbr[k]})

    def wt_in(j, k):
        return rc(wf.at[j, part(nbr[k])], wf.at[j, part(nbr[k])], wt_s.at[j, k], wt_r.at[j, k], {"tok": nbr[k]})

    def wd(j, k):
        piece = wf.at[j, subpart(nbr[k], k)]
        return rc(piece, piece, wt_s.at[j, 2 + k], wt_r.at[j, 2 + k], {"tok": nbr[1 - k]})

    def wd_in(j, k):
        piece = wf.at[j, subpart(diag, k)]
        return rc(piece, piece, wt_s.at[j, 2 + k], wt_r.at[j, 2 + k], {"tok": nbr[1 - k]})

    def y_send(src, i, g, c, k, dev):
        return rc(src.at[group(c, g)], tg.at[i, group(c, g)], th_s.at[k, 2 * g + c], th_r.at[i, 2 * g + c], {"voc": dev})

    def y_own(g, c, k, dev):
        return y_send(y_hbm, z, g, c, k, dev)

    def y_relay(i, g, c, k):
        return y_send(tg.at[i], i, g, c, k, outer)

    def y_out(g, k, dev, cs=(0, 1)):
        for c in cs:
            y_own(g, c, k, dev).start()

    @pl.when(at_end)
    def _():
        for j in (near, mid, far):
            wz(j).start()
        y_out(0, 0, near)

    @pl.when(inside)
    def _():
        for j in (outer, inner, beyond):
            wz(j).start()
        y_out(0, 1, outer)
        y_out(0, 0, inner)
        for g in range(1, ng):
            y_out(g, 1, outer)
            y_out(g, 0, inner)

    for k in range(n):
        tw_copy(zdev(k)).start()

    for c in ins:
        c.wait()
    wcol[...] = jnp.transpose(jnp.broadcast_to(w_ref[...], (rows, rows)))

    def w_arrive(j):
        wz_in(j).wait_recv()
        for k in range(2):
            wt(j, k).start()

    def w_spread(j):
        for k in range(2):
            wt_in(j, k).wait_recv()
            wd(j, k).start()

    def teacher_dot(src, i, g, first):
        step = kt // 2

        @pl.loop(0, 2)
        def _(s):
            cols = pl.ds(pl.multiple_of(s * step, step), step)
            both = jnp.concatenate([src[pl.ds(c * half + g * q, q), cols] for c in range(2)], axis=0)
            term = jnp.dot(both, tw[i, cols, :], preferred_element_type=F32)
            if first:
                @pl.when(s == 0)
                def _():
                    tacc[g] = term

                @pl.when(s > 0)
                def _():
                    tacc[g] += term
            else:
                tacc[g] += term

    def take_y(i, g, c, k=None):
        y_send(tg.at[i], i, g, c, 0, outer).wait_recv()
        if k is not None:
            y_relay(i, g, c, k).start()

    def dot_y(i, g):
        teacher_dot(tg.at[i], i, g, False)

    def full_y(i, g, k=None):
        for c in range(2):
            take_y(i, g, c, k)
        dot_y(i, g)

    def student(j):
        sp[j] = jnp.dot(x_ref[...], wf[j], preferred_element_type=F32)
        rc(sp.at[j, theirs], spx.at[j], px_s.at[j], px_r.at[j], partner).start()

    def student_sum(j):
        rc(sp.at[j, theirs], spx.at[j], px_s.at[j], px_r.at[j], partner).wait_recv()
        ssum[j] = sp[j, mine, :] + spx[j]

    def rs(side, j):
        return rc(ssum.at[j], srr.at[side, j], rs_s.at[j], rs_r.at[side, j], {"voc": z + 2 * side - 1})

    def student_full(j):
        for k in range(2):
            wd_in(j, k).wait_recv()
        student(j)

    def rs_take(side, j):
        rs(side, j).wait_recv()
        ssum[j] += srr[side, j]

    def student_pass(j, side, upstream):
        student_sum(j)
        if upstream:
            rs_take(side, j)
        rs(side, j).start()

    def t_swap(g):
        return rc(tacc.at[g, pl.ds(pl.multiple_of((1 - h) * q, q), q)], tpx.at[g], tx_s.at[g], tx_r.at[g], partner)

    def stx(g, j, src):
        return rc(stat.at[g, src], stat.at[g, src], st_s.at[g, j], st_r.at[g, src], {"voc": j})

    def gz(g, j, src):
        return rc(gap.at[src, group(h, g)], gap.at[src, group(h, g)], gz_s.at[g, j], gz_r.at[g, src], {"voc": j})

    def gx(g, src, c):
        return rc(gap.at[src, group(c, g)], gap.at[src, group(c, g)], gx_s.at[g, src], gx_r.at[g, src], partner)

    def send_stats(g):
        t_swap(g).wait_recv()
        tl = tacc[g, pl.ds(pl.multiple_of(h * q, q), q), :] + tpx[g]
        tpx[g] = tl
        sl = ssum[z, pl.ds(g * q, q), :]
        ms = jnp.max(sl, axis=1, keepdims=True)
        ss = jnp.sum(jnp.exp(sl - ms), axis=1, keepdims=True)
        mt = jnp.max(tl, axis=1, keepdims=True)
        et = jnp.exp(tl - mt)
        st = jnp.sum(et, axis=1, keepdims=True)
        cr = jnp.sum(et * (tl - sl), axis=1, keepdims=True)
        lane = lax.broadcasted_iota(jnp.int32, (q, 128), 1)
        cols = jnp.where(lane == 0, ms, jnp.where(lane == 1, mt, jnp.where(
            lane == 2, ss, jnp.where(lane == 3, st, cr))))
        stat[g, z] = jnp.transpose(jnp.concatenate([cols] * (128 // q), axis=0))[:8]
        for k in (2, 1, 3):
            stx(g, zdev(k), z).start()

    def send_gap(g):
        for k in range(1, n):
            stx(g, zdev(k), zdev(k)).wait_recv()
        parts = [stat[g, j] for j in range(n)]
        top = parts[0]
        for p in parts[1:]:
            top = jnp.maximum(top, p)
        big_s, big_t = top[0:1], top[1:2]
        tot_s = jnp.zeros_like(big_s)
        tot_t = jnp.zeros_like(big_s)
        cross = jnp.zeros_like(big_s)
        for p in parts:
            es = jnp.exp(p[0:1] - big_s)
            ets = jnp.exp(p[1:2] - big_t)
            tot_s = tot_s + p[2:3] * es
            tot_t = tot_t + p[3:4] * ets
            cross = cross + p[4:5] * ets
        lse_s = big_s + jnp.log(tot_s)
        lse_t = big_t + jnp.log(tot_t)
        scale = wcol[group(h, g), :][:, 0:1]
        sub = lax.broadcasted_iota(jnp.int32, (128, 128), 0)
        back = jnp.transpose(jnp.where(sub == 0, lse_s, lse_t))[:q]
        col_s, col_t = back[:, 0:1], back[:, 1:2]
        sl = ssum[z, pl.ds(g * q, q), :]
        gap[z, group(h, g), :] = (scale * (jnp.exp(sl - col_s) - jnp.exp(tpx[g] - col_t))).astype(BF16)
        for k in (2, 1, 3):
            gz(g, zdev(k), z).start()
        gx(g, z, h).start()
        div = cross / tot_t - lse_t + lse_s
        first = lax.broadcasted_iota(jnp.int32, div.shape, 1) < q
        lossr[g] = jnp.broadcast_to(jnp.sum(jnp.where(first, div, 0.0), axis=1, keepdims=True), (8, 128))

    def take_gap(g, j):
        gz(g, j, j).wait_recv()
        gx(g, j, h).start()

    def grad_dot(g, j, first):
        gx(g, j, 1 - h).wait_recv()
        both = jnp.concatenate([gap[j, pl.ds(c * half + g * q, q), :] for c in range(2)], axis=0)
        term = lax.dot_general(both, wf[j], (((1,), (1,)), ((), ())), preferred_element_type=F32)
        if first:
            acc[g] = term
        else:
            acc[g] += term

    def out_copy(g, c):
        rows_gc = pl.ds(c * half + g * q, q)
        return pltpu.make_async_copy(stage.at[rows_gc], out.at[rows_gc], oc.at[2 * g + c])

    def store(g):
        for c in range(2):
            stage[pl.ds(c * half + g * q, q), :] = acc[g, pl.ds(c * q, q), :].astype(BF16)
            out_copy(g, c).start()

    def drain_bulk():
        for k in range(1, n):
            j = zdev(k)
            wz(j).wait_send()
            for b in range(2):
                wt(j, b).wait_send()
                wd(j, b).wait_send()
            rs(side_in, j).wait_send()
        for g in range(ng):
            for c in range(2):
                y_own(g, c, 0, near).wait_send()

                @pl.when(at_end)
                def _(g=g, c=c):
                    y_own(g, c, 1, mid).wait_send()

                @pl.when(inside)
                def _(g=g, c=c):
                    y_own(g, c, 1, outer).wait_send()
                    for k, j in ((2, beyond), (3, inner)):
                        y_relay(j, g, c, k).wait_send()
            t_swap(g).wait_send()
        for j in range(n):
            rc(sp.at[j, theirs], spx.at[j], px_s.at[j], px_r.at[j], partner).wait_send()

    def local_dots():
        for i in range(n):
            tw_copy(i).wait()
        for g in range(ng):
            teacher_dot(y_ref, z, g, True)
        own_w.wait()
        student(z)

    @pl.when(at_end)
    def _():
        w_arrive(near)
        local_dots()
        w_spread(near)
        student_full(near)
        w_arrive(far)
        w_spread(far)
        y_out(0, 1, mid)
        student_pass(near, side_in, False)
        w_arrive(mid)
        student_full(far)
        full_y(near, 0)
        student_pass(far, side_in, False)
        w_spread(mid)
        full_y(near, 1)
        student_full(mid)

        @pl.when(h == 1)
        def _():
            y_out(1, 1, mid)
        student_sum(z)
        student_pass(mid, side_in, False)

        @pl.when(h == 0)
        def _():
            y_out(1, 1, mid)
        y_out(1, 0, near)
        full_y(far, 0)
        full_y(mid, 0)
        t_swap(0).start()
        full_y(mid, 1)
        rs_take(side_out, z)
        send_stats(0)
        full_y(far, 1)
        t_swap(1).start()

    @pl.when(inside)
    def _():
        w_arrive(outer)
        local_dots()
        w_spread(outer)
        w_arrive(inner)
        w_arrive(beyond)
        student_full(outer)
        w_spread(inner)
        w_spread(beyond)
        take_y(inner, 0, 0, 3)
        take_y(beyond, 0, 0, 2)
        student_full(inner)
        take_y(beyond, 0, 1, 2)
        dot_y(beyond, 0)
        full_y(outer, 0)
        take_y(inner, 0, 1, 3)
        student_full(beyond)
        student_pass(beyond, side_in, True)
        dot_y(inner, 0)
        t_swap(0).start()
        take_y(inner, 1, 0, 3)
        take_y(inner, 1, 1, 3)

        @pl.when(h == 1)
        def _():
            take_y(beyond, 1, 0, 2)
            take_y(beyond, 1, 1, 2)
            student_pass(outer, side_out, True)
            student_pass(inner, side_in, True)

        @pl.when(h == 0)
        def _():
            student_pass(outer, side_out, True)
            take_y(beyond, 1, 0, 2)
            student_pass(inner, side_in, True)
            take_y(beyond, 1, 1, 2)
        dot_y(inner, 1)
        dot_y(beyond, 1)
        student_sum(z)
        rs_take(side_in, z)
        rs_take(side_out, z)
        send_stats(0)
        full_y(outer, 1)
        t_swap(1).start()

    def lp():
        return rc(lossb.at[0], lossb.at[1], ls_s.at[nt], ls_r.at[nt], partner)

    def ls(a, b):
        return rc(lossx.at[b], lossx.at[b], ls_s.at[a], ls_r.at[b], {"tok": a})

    send_stats(1)
    send_gap(0)
    drain_bulk()
    send_gap(1)
    lossb[0] = lossr[0] + lossr[1]
    lp().start()
    across = lax.rem(z + 2, n)
    order = (near, across, n * (n - 1) // 2 - z - near - across)
    grad_dot(0, z, True)
    for j in order:
        take_gap(0, j)
    lp().wait_recv()
    lossx[t] = lossb[0] + lossb[1]
    for k in range(1, nt):
        ls(lax.rem(t + k, nt), t).start()
    grad_dot(1, z, True)
    for j in order:
        grad_dot(0, j, False)
    store(0)
    for j in order:
        take_gap(1, j)
    for j in order:
        grad_dot(1, j, False)
    store(1)
    for k in range(1, nt):
        ls(t, lax.rem(t + k, nt)).wait_recv()
    total = lossx[0]
    for a in range(1, nt):
        total = total + lossx[a]
    loss_out[0, 0] = total[0, 0] / (rows * nt)

    for g in range(ng):
        for k in range(1, n):
            stx(g, zdev(k), z).wait_send()
            gz(g, zdev(k), z).wait_send()
        for j in range(n):
            gx(g, j, h).wait_send()
    lp().wait_send()
    for k in range(1, nt):
        ls(lax.rem(t + k, nt), t).wait_send()
    for g in range(ng):
        for c in range(2):
            out_copy(g, c).wait()


def fused_shards(n, nt, student_hidden, teacher_hidden, student_head, teacher_head, loss_weight):
    rows, ks = student_hidden.shape
    kt = teacher_hidden.shape[1]
    v = student_head.shape[1]
    half = rows // 2
    ng = GROUPS
    q = half // ng
    dma = lambda *s: pltpu.SemaphoreType.DMA(s)
    vmem = lambda s, d: pltpu.VMEM(s, d)
    anywhere = pl.BlockSpec(memory_space=pl.ANY)
    grad, loss = pl.pallas_call(
        functools.partial(fused, n, nt, ng),
        out_shape=(jax.ShapeDtypeStruct((rows, ks), BF16), jax.ShapeDtypeStruct((1, 1), F32)),
        in_specs=[anywhere] * 5,
        out_specs=(anywhere, pl.BlockSpec(memory_space=pltpu.SMEM)),
        scratch_shapes=[
            vmem((rows, ks), BF16),
            vmem((rows, kt), BF16),
            vmem((1, rows), F32),
            vmem((n, ks, v), BF16),
            vmem((n, kt, v), BF16),
            vmem((n, rows, kt), BF16),
            vmem((n, rows, v), F32),
            vmem((n, half, v), F32),
            vmem((n, half, v), F32),
            vmem((2, n, half, v), F32),
            vmem((ng, 2 * q, v), F32),
            vmem((ng, q, v), F32),
            vmem((ng, n, 8, 128), F32),
            vmem((n, rows, v), BF16),
            vmem((rows, rows), F32),
            vmem((2, 8, 128), F32),
            vmem((ng, 8, 128), F32),
            vmem((nt, 8, 128), F32),
            vmem((ng, 2 * q, ks), F32),
            vmem((rows, ks), BF16),
            dma(n + 4),
            dma(n), dma(n), dma(n, 4), dma(n, 4),
            dma(4, 2 * ng), dma(n, 2 * ng),
            dma(n), dma(n), dma(ng), dma(ng), dma(n), dma(2, n),
            dma(ng, n), dma(ng, n), dma(ng, n), dma(ng, n), dma(ng, n), dma(ng, n),
            dma(nt + 1), dma(nt + 1), dma(2 * ng),
        ],
        compiler_params=pltpu.CompilerParams(
            collective_id=0, has_side_effects=True, vmem_limit_bytes=60 << 20),
        name="divergence_grad",
    )(student_hidden, teacher_hidden, loss_weight.reshape(1, rows), student_head, teacher_head)
    return grad, loss.reshape(())


def divergence_terms(student_logits, teacher_logits, weights):
    differences = teacher_logits - student_logits
    peak_student, peak_teacher = lax.pmax(
        (jnp.max(student_logits, axis=1), jnp.max(teacher_logits, axis=1)), "voc"
    )
    scaled_student = jnp.exp(student_logits - peak_student[:, None])
    scaled_teacher = jnp.exp(teacher_logits - peak_teacher[:, None])
    total_student, total_teacher, cross_sum = lax.psum(
        (
            jnp.sum(scaled_student, axis=1),
            jnp.sum(scaled_teacher, axis=1),
            jnp.sum(scaled_teacher * differences, axis=1),
        ),
        "voc",
    )
    student_lse = peak_student + jnp.log(total_student)
    teacher_lse = peak_teacher + jnp.log(total_teacher)
    divergence = cross_sum / total_teacher - teacher_lse + student_lse
    prob_gap = jnp.exp(student_logits - student_lse[:, None]) - jnp.exp(
        teacher_logits - teacher_lse[:, None]
    )
    scaled_gap = (weights[:, None] * prob_gap).astype(jnp.bfloat16)
    return (divergence, scaled_gap)


def plain_shards(student_hidden, teacher_hidden, student_head, teacher_head, loss_weight):
    student_block, teacher_block = (
        lax.all_gather(student_hidden, "voc", axis=1, tiled=True),
        lax.all_gather(teacher_hidden, "voc", axis=1, tiled=True),
    )
    vocab_local = student_head.shape[1]
    row_count = student_block.shape[0] // lax.axis_size("hid")
    joined = lax.psum_scatter(
        jnp.concatenate(
            [
                jnp.dot(student_block, student_head, preferred_element_type=jnp.float32),
                jnp.dot(teacher_block, teacher_head, preferred_element_type=jnp.float32),
            ],
            axis=1,
        ),
        "hid",
        scatter_dimension=0,
        tiled=True,
    )
    student_logits = joined[:, :vocab_local]
    teacher_logits = joined[:, vocab_local:]
    weights = lax.dynamic_slice_in_dim(loss_weight, lax.axis_index("hid") * row_count, row_count)
    divergence, scaled_gap = divergence_terms(student_logits, teacher_logits, weights)
    token_total = loss_weight.shape[0] * lax.axis_size("tok")
    loss_total = lax.psum(jnp.sum(divergence), ("tok", "hid"))
    grad_terms = lax.dot_general(
        lax.all_gather(scaled_gap, "hid", axis=0, tiled=True),
        student_head,
        (((1,), (1,)), ((), ())),
        preferred_element_type=jnp.float32,
    )
    grad_hidden = lax.psum_scatter(grad_terms, "voc", scatter_dimension=1, tiled=True).astype(
        jnp.bfloat16
    )
    mean_loss = loss_total / token_total
    return (grad_hidden, mean_loss)


def solution(mesh):
    placed = (
        P("tok", ("hid", "voc")),
        P("tok", ("hid", "voc")),
        P("hid", "voc"),
        P("hid", "voc"),
        P("tok"),
    )
    n, nt = mesh.shape["voc"], mesh.shape["tok"]
    if n == 4 and nt == 4 and mesh.shape["hid"] == 2:
        body = functools.partial(fused_shards, n, nt)
    else:
        body = plain_shards
    return jax.shard_map(
        body,
        mesh=mesh,
        in_specs=placed,
        out_specs=(P("tok", ("hid", "voc")), P()),
        check_vma=False,
    )
```

```python
import functools

import jax
import jax.numpy as jnp
from jax import lax
from jax.experimental import pallas as pl
from jax.experimental.pallas import tpu as pltpu
from jax.sharding import PartitionSpec as P

MESH = pl.DeviceIdType.MESH
F32 = jnp.float32
BF16 = jnp.bfloat16
GROUPS = 2


def fused(n, nt, ng, x_hbm, y_hbm, w_hbm, sw_hbm, tw_hbm, out, loss_out,
          x_ref, y_ref, w_ref, wf, tw, tg, sp, spx, ssum, srr, tacc, tpx, stat, gap, wcol, lossb, lossr, lossx, acc,
          lc, wz_s, wz_r, wt_s, wt_r, th_s, th_r, px_s, px_r, tx_s, tx_r, rs_s, rs_r,
          st_s, st_r, gz_s, gz_r, gx_s, gx_r, ls_s, ls_r):
    z = lax.axis_index("voc")
    t = lax.axis_index("tok")
    h = lax.axis_index("hid")
    rows, ks = x_ref.shape
    kt = y_ref.shape[1]
    half = rows // 2
    q = half // ng
    quarter = ks // nt
    eighth = quarter // 2
    partner = {"hid": 1 - h}
    mine = pl.ds(pl.multiple_of(h * half, half), half)
    theirs = pl.ds(pl.multiple_of((1 - h) * half, half), half)
    nbr = (t + 1 - 2 * lax.rem(t, 2), lax.rem(t + 2, 4))
    diag = nt - 1 - t
    at_end = jnp.logical_or(z == 0, z == n - 1)
    inside = jnp.logical_not(at_end)
    side_in = jnp.where(z < n // 2, 1, 0)
    side_out = 1 - side_in
    step_in = 2 * side_in - 1
    near, mid, far = z + step_in, z + 2 * step_in, z + 3 * step_in
    inner, beyond, outer = z + step_in, z + 2 * step_in, z - step_in

    def rc(src, dst, ss, rs, dev):
        return pltpu.make_async_remote_copy(
            src_ref=src, dst_ref=dst, send_sem=ss, recv_sem=rs,
            device_id=dev, device_id_type=MESH)

    def zdev(k):
        return lax.rem(z + k, n)

    def group(c, g):
        return pl.ds(pl.multiple_of(c * half + g * q, q), q)

    own_w = pltpu.make_async_copy(sw_hbm.at[pl.ds(pl.multiple_of(z * ks, ks), ks)], wf.at[z], lc.at[n])
    own_w.start()
    ins = [pltpu.make_async_copy(a, b, lc.at[n + 1 + i])
           for i, (a, b) in enumerate(((x_hbm, x_ref), (y_hbm, y_ref), (w_hbm, w_ref)))]
    for c in ins:
        c.start()

    def tw_copy(i):
        return pltpu.make_async_copy(tw_hbm.at[pl.ds(pl.multiple_of(i * kt, kt), kt)], tw.at[i], lc.at[i])

    barrier = pltpu.get_barrier_semaphore()
    for k in range(1, n):
        pl.semaphore_signal(barrier, inc=1, device_id={"voc": zdev(k)}, device_id_type=MESH)
    for k in range(1, nt):
        pl.semaphore_signal(barrier, inc=1, device_id={"tok": lax.rem(t + k, nt)}, device_id_type=MESH)
    pl.semaphore_signal(barrier, inc=1, device_id=partner, device_id_type=MESH)
    pl.semaphore_wait(barrier, n - 1 + nt - 1 + 1)

    def part(i):
        return pl.ds(pl.multiple_of(i * quarter, quarter), quarter)

    def subpart(i, b):
        return pl.ds(pl.multiple_of(i * quarter + b * eighth, eighth), eighth)

    def wz(j):
        return rc(sw_hbm.at[pl.ds(pl.multiple_of(j * ks + t * quarter, quarter), quarter)],
                  wf.at[z, part(t)], wz_s.at[j], wz_r.at[z], {"voc": j})

    def wz_in(j):
        return rc(wf.at[j, part(t)], wf.at[j, part(t)], wz_s.at[j], wz_r.at[j], {"voc": j})

    def wt(j, k):
        return rc(wf.at[j, part(t)], wf.at[j, part(t)], wt_s.at[j, k], wt_r.at[j, k], {"tok": nbr[k]})

    def wt_in(j, k):
        return rc(wf.at[j, part(nbr[k])], wf.at[j, part(nbr[k])], wt_s.at[j, k], wt_r.at[j, k], {"tok": nbr[k]})

    def wd(j, k):
        piece = wf.at[j, subpart(nbr[k], k)]
        return rc(piece, piece, wt_s.at[j, 2 + k], wt_r.at[j, 2 + k], {"tok": nbr[1 - k]})

    def wd_in(j, k):
        piece = wf.at[j, subpart(diag, k)]
        return rc(piece, piece, wt_s.at[j, 2 + k], wt_r.at[j, 2 + k], {"tok": nbr[1 - k]})

    def y_send(src, i, g, c, k, dev):
        return rc(src.at[group(c, g)], tg.at[i, group(c, g)], th_s.at[k, 2 * g + c], th_r.at[i, 2 * g + c], {"voc": dev})

    def y_own(g, c, k, dev):
        return y_send(y_hbm, z, g, c, k, dev)

    def y_relay(i, g, c, k):
        return y_send(tg.at[i], i, g, c, k, outer)

    def y_out(g, k, dev, cs=(0, 1)):
        for c in cs:
            y_own(g, c, k, dev).start()

    @pl.when(at_end)
    def _():
        for j in (near, mid, far):
            wz(j).start()
        y_out(0, 0, near)

    @pl.when(inside)
    def _():
        for j in (outer, inner, beyond):
            wz(j).start()
        y_out(0, 1, outer)
        y_out(0, 0, inner)
        for g in range(1, ng):
            y_out(g, 1, outer)
            y_out(g, 0, inner)

    for k in range(n):
        tw_copy(zdev(k)).start()

    for c in ins:
        c.wait()
    wcol[...] = jnp.transpose(jnp.broadcast_to(w_ref[...], (rows, rows)))

    def w_arrive(j):
        wz_in(j).wait_recv()
        for k in range(2):
            wt(j, k).start()

    def w_spread(j):
        for k in range(2):
            wt_in(j, k).wait_recv()
            wd(j, k).start()

    def teacher_dot(src, i, g, first):
        step = kt // 2

        @pl.loop(0, 2)
        def _(s):
            cols = pl.ds(pl.multiple_of(s * step, step), step)
            both = jnp.concatenate([src[pl.ds(c * half + g * q, q), cols] for c in range(2)], axis=0)
            term = jnp.dot(both, tw[i, cols, :], preferred_element_type=F32)
            if first:
                @pl.when(s == 0)
                def _():
                    tacc[g] = term

                @pl.when(s > 0)
                def _():
                    tacc[g] += term
            else:
                tacc[g] += term

    def take_y(i, g, c, k=None):
        y_send(tg.at[i], i, g, c, 0, outer).wait_recv()
        if k is not None:
            y_relay(i, g, c, k).start()

    def dot_y(i, g):
        teacher_dot(tg.at[i], i, g, False)

    def full_y(i, g, k=None):
        for c in range(2):
            take_y(i, g, c, k)
        dot_y(i, g)

    def student(j):
        sp[j] = jnp.dot(x_ref[...], wf[j], preferred_element_type=F32)
        rc(sp.at[j, theirs], spx.at[j], px_s.at[j], px_r.at[j], partner).start()

    def student_sum(j):
        rc(sp.at[j, theirs], spx.at[j], px_s.at[j], px_r.at[j], partner).wait_recv()
        ssum[j] = sp[j, mine, :] + spx[j]

    def rs(side, j):
        return rc(ssum.at[j], srr.at[side, j], rs_s.at[j], rs_r.at[side, j], {"voc": z + 2 * side - 1})

    def student_full(j):
        for k in range(2):
            wd_in(j, k).wait_recv()
        student(j)

    def rs_take(side, j):
        rs(side, j).wait_recv()
        ssum[j] += srr[side, j]

    def student_pass(j, side, upstream):
        student_sum(j)
        if upstream:
            rs_take(side, j)
        rs(side, j).start()

    def t_swap(g):
        return rc(tacc.at[g, pl.ds(pl.multiple_of((1 - h) * q, q), q)], tpx.at[g], tx_s.at[g], tx_r.at[g], partner)

    def stx(g, j, src):
        return rc(stat.at[g, src], stat.at[g, src], st_s.at[g, j], st_r.at[g, src], {"voc": j})

    def gz(g, j, src):
        return rc(gap.at[src, group(h, g)], gap.at[src, group(h, g)], gz_s.at[g, j], gz_r.at[g, src], {"voc": j})

    def gx(g, src, c):
        return rc(gap.at[src, group(c, g)], gap.at[src, group(c, g)], gx_s.at[g, src], gx_r.at[g, src], partner)

    def send_stats(g):
        t_swap(g).wait_recv()
        tl = tacc[g, pl.ds(pl.multiple_of(h * q, q), q), :] + tpx[g]
        tpx[g] = tl
        sl = ssum[z, pl.ds(g * q, q), :]
        ms = jnp.max(sl, axis=1, keepdims=True)
        ss = jnp.sum(jnp.exp(sl - ms), axis=1, keepdims=True)
        mt = jnp.max(tl, axis=1, keepdims=True)
        et = jnp.exp(tl - mt)
        st = jnp.sum(et, axis=1, keepdims=True)
        cr = jnp.sum(et * (tl - sl), axis=1, keepdims=True)
        lane = lax.broadcasted_iota(jnp.int32, (q, 128), 1)
        cols = jnp.where(lane == 0, ms, jnp.where(lane == 1, mt, jnp.where(
            lane == 2, ss, jnp.where(lane == 3, st, cr))))
        stat[g, z] = jnp.transpose(jnp.concatenate([cols] * (128 // q), axis=0))[:8]
        for k in (2, 1, 3):
            stx(g, zdev(k), z).start()

    def send_gap(g):
        for k in range(1, n):
            stx(g, zdev(k), zdev(k)).wait_recv()
        parts = [stat[g, j] for j in range(n)]
        top = parts[0]
        for p in parts[1:]:
            top = jnp.maximum(top, p)
        big_s, big_t = top[0:1], top[1:2]
        tot_s = jnp.zeros_like(big_s)
        tot_t = jnp.zeros_like(big_s)
        cross = jnp.zeros_like(big_s)
        for p in parts:
            es = jnp.exp(p[0:1] - big_s)
            ets = jnp.exp(p[1:2] - big_t)
            tot_s = tot_s + p[2:3] * es
            tot_t = tot_t + p[3:4] * ets
            cross = cross + p[4:5] * ets
        lse_s = big_s + jnp.log(tot_s)
        lse_t = big_t + jnp.log(tot_t)
        scale = wcol[group(h, g), :][:, 0:1]
        sub = lax.broadcasted_iota(jnp.int32, (128, 128), 0)
        back = jnp.transpose(jnp.where(sub == 0, lse_s, lse_t))[:q]
        col_s, col_t = back[:, 0:1], back[:, 1:2]
        sl = ssum[z, pl.ds(g * q, q), :]
        gap[z, group(h, g), :] = (scale * (jnp.exp(sl - col_s) - jnp.exp(tpx[g] - col_t))).astype(BF16)
        for k in (2, 1, 3):
            gz(g, zdev(k), z).start()
        gx(g, z, h).start()
        div = cross / tot_t - lse_t + lse_s
        first = lax.broadcasted_iota(jnp.int32, div.shape, 1) < q
        lossr[g] = jnp.broadcast_to(jnp.sum(jnp.where(first, div, 0.0), axis=1, keepdims=True), (8, 128))

    def take_gap(g, j):
        gz(g, j, j).wait_recv()
        gx(g, j, h).start()

    def grad_dot(g, j, first):
        gx(g, j, 1 - h).wait_recv()
        both = jnp.concatenate([gap[j, pl.ds(c * half + g * q, q), :] for c in range(2)], axis=0)
        term = lax.dot_general(both, wf[j], (((1,), (1,)), ((), ())), preferred_element_type=F32)
        if first:
            acc[g] = term
        else:
            acc[g] += term

    def store(g):
        for c in range(2):
            out[pl.ds(c * half + g * q, q), :] = acc[g, pl.ds(c * q, q), :].astype(BF16)

    def drain_bulk():
        for k in range(1, n):
            j = zdev(k)
            wz(j).wait_send()
            for b in range(2):
                wt(j, b).wait_send()
                wd(j, b).wait_send()
            rs(side_in, j).wait_send()
        for g in range(ng):
            for c in range(2):
                y_own(g, c, 0, near).wait_send()

                @pl.when(at_end)
                def _(g=g, c=c):
                    y_own(g, c, 1, mid).wait_send()

                @pl.when(inside)
                def _(g=g, c=c):
                    y_own(g, c, 1, outer).wait_send()
                    for k, j in ((2, beyond), (3, inner)):
                        y_relay(j, g, c, k).wait_send()
            t_swap(g).wait_send()
        for j in range(n):
            rc(sp.at[j, theirs], spx.at[j], px_s.at[j], px_r.at[j], partner).wait_send()

    def local_dots():
        for i in range(n):
            tw_copy(i).wait()
        for g in range(ng):
            teacher_dot(y_ref, z, g, True)
        own_w.wait()
        student(z)

    @pl.when(at_end)
    def _():
        w_arrive(near)
        local_dots()
        w_spread(near)
        student_full(near)
        w_arrive(far)
        w_spread(far)
        y_out(0, 1, mid)
        student_pass(near, side_in, False)
        w_arrive(mid)
        student_full(far)
        full_y(near, 0)
        student_pass(far, side_in, False)
        w_spread(mid)
        full_y(near, 1)
        student_full(mid)

        @pl.when(h == 1)
        def _():
            y_out(1, 1, mid)
        student_sum(z)
        student_pass(mid, side_in, False)

        @pl.when(h == 0)
        def _():
            y_out(1, 1, mid)
        y_out(1, 0, near)
        full_y(far, 0)
        full_y(mid, 0)
        t_swap(0).start()
        full_y(mid, 1)
        rs_take(side_out, z)
        send_stats(0)
        full_y(far, 1)
        t_swap(1).start()

    @pl.when(inside)
    def _():
        w_arrive(outer)
        local_dots()
        w_spread(outer)
        w_arrive(inner)
        w_arrive(beyond)
        student_full(outer)
        w_spread(inner)
        w_spread(beyond)
        take_y(inner, 0, 0, 3)
        take_y(beyond, 0, 0, 2)
        student_full(inner)
        take_y(beyond, 0, 1, 2)
        dot_y(beyond, 0)
        full_y(outer, 0)
        take_y(inner, 0, 1, 3)
        student_full(beyond)
        student_pass(beyond, side_in, True)
        dot_y(inner, 0)
        t_swap(0).start()
        take_y(inner, 1, 0, 3)
        take_y(inner, 1, 1, 3)

        @pl.when(h == 1)
        def _():
            take_y(beyond, 1, 0, 2)
            take_y(beyond, 1, 1, 2)
            student_pass(outer, side_out, True)
            student_pass(inner, side_in, True)

        @pl.when(h == 0)
        def _():
            student_pass(outer, side_out, True)
            take_y(beyond, 1, 0, 2)
            student_pass(inner, side_in, True)
            take_y(beyond, 1, 1, 2)
        dot_y(inner, 1)
        dot_y(beyond, 1)
        student_sum(z)
        rs_take(side_in, z)
        rs_take(side_out, z)
        send_stats(0)
        full_y(outer, 1)
        t_swap(1).start()

    def lp():
        return rc(lossb.at[0], lossb.at[1], ls_s.at[nt], ls_r.at[nt], partner)

    def ls(a, b):
        return rc(lossx.at[b], lossx.at[b], ls_s.at[a], ls_r.at[b], {"tok": a})

    send_stats(1)
    send_gap(0)
    drain_bulk()
    send_gap(1)
    lossb[0] = lossr[0] + lossr[1]
    lp().start()
    across = lax.rem(z + 2, n)
    order = (near, across, n * (n - 1) // 2 - z - near - across)
    grad_dot(0, z, True)
    for j in order:
        take_gap(0, j)
    lp().wait_recv()
    lossx[t] = lossb[0] + lossb[1]
    for k in range(1, nt):
        ls(lax.rem(t + k, nt), t).start()
    grad_dot(1, z, True)
    for j in order:
        grad_dot(0, j, False)
    store(0)
    for j in order:
        take_gap(1, j)
    for j in order:
        grad_dot(1, j, False)
    store(1)
    for k in range(1, nt):
        ls(t, lax.rem(t + k, nt)).wait_recv()
    total = lossx[0]
    for a in range(1, nt):
        total = total + lossx[a]
    loss_out[0, 0] = total[0, 0] / (rows * nt)

    for g in range(ng):
        for k in range(1, n):
            stx(g, zdev(k), z).wait_send()
            gz(g, zdev(k), z).wait_send()
        for j in range(n):
            gx(g, j, h).wait_send()
    lp().wait_send()
    for k in range(1, nt):
        ls(lax.rem(t + k, nt), t).wait_send()


def fused_shards(n, nt, student_hidden, teacher_hidden, student_head, teacher_head, loss_weight):
    rows, ks = student_hidden.shape
    kt = teacher_hidden.shape[1]
    v = student_head.shape[1]
    half = rows // 2
    ng = GROUPS
    q = half // ng
    dma = lambda *s: pltpu.SemaphoreType.DMA(s)
    vmem = lambda s, d: pltpu.VMEM(s, d)
    anywhere = pl.BlockSpec(memory_space=pl.ANY)
    grad, loss = pl.pallas_call(
        functools.partial(fused, n, nt, ng),
        out_shape=(pltpu.VMEM((rows, ks), BF16), pltpu.SMEM((1, 1), F32)),
        in_specs=[anywhere] * 5,
        out_specs=(pl.BlockSpec(memory_space=pltpu.VMEM), pl.BlockSpec(memory_space=pltpu.SMEM)),
        scratch_shapes=[
            vmem((rows, ks), BF16),
            vmem((rows, kt), BF16),
            vmem((1, rows), F32),
            vmem((n, ks, v), BF16),
            vmem((n, kt, v), BF16),
            vmem((n, rows, kt), BF16),
            vmem((n, rows, v), F32),
            vmem((n, half, v), F32),
            vmem((n, half, v), F32),
            vmem((2, n, half, v), F32),
            vmem((ng, 2 * q, v), F32),
            vmem((ng, q, v), F32),
            vmem((ng, n, 8, 128), F32),
            vmem((n, rows, v), BF16),
            vmem((rows, rows), F32),
            vmem((2, 8, 128), F32),
            vmem((ng, 8, 128), F32),
            vmem((nt, 8, 128), F32),
            vmem((ng, 2 * q, ks), F32),
            dma(n + 4),
            dma(n), dma(n), dma(n, 4), dma(n, 4),
            dma(4, 2 * ng), dma(n, 2 * ng),
            dma(n), dma(n), dma(ng), dma(ng), dma(n), dma(2, n),
            dma(ng, n), dma(ng, n), dma(ng, n), dma(ng, n), dma(ng, n), dma(ng, n),
            dma(nt + 1), dma(nt + 1),
        ],
        compiler_params=pltpu.CompilerParams(
            collective_id=0, has_side_effects=True, vmem_limit_bytes=60 << 20),
        name="divergence_grad",
    )(student_hidden, teacher_hidden, loss_weight.reshape(1, rows), student_head, teacher_head)
    return grad, loss.reshape(())


def divergence_terms(student_logits, teacher_logits, weights):
    differences = teacher_logits - student_logits
    peak_student, peak_teacher = lax.pmax(
        (jnp.max(student_logits, axis=1), jnp.max(teacher_logits, axis=1)), "voc"
    )
    scaled_student = jnp.exp(student_logits - peak_student[:, None])
    scaled_teacher = jnp.exp(teacher_logits - peak_teacher[:, None])
    total_student, total_teacher, cross_sum = lax.psum(
        (
            jnp.sum(scaled_student, axis=1),
            jnp.sum(scaled_teacher, axis=1),
            jnp.sum(scaled_teacher * differences, axis=1),
        ),
        "voc",
    )
    student_lse = peak_student + jnp.log(total_student)
    teacher_lse = peak_teacher + jnp.log(total_teacher)
    divergence = cross_sum / total_teacher - teacher_lse + student_lse
    prob_gap = jnp.exp(student_logits - student_lse[:, None]) - jnp.exp(
        teacher_logits - teacher_lse[:, None]
    )
    scaled_gap = (weights[:, None] * prob_gap).astype(jnp.bfloat16)
    return (divergence, scaled_gap)


def plain_shards(student_hidden, teacher_hidden, student_head, teacher_head, loss_weight):
    student_block, teacher_block = (
        lax.all_gather(student_hidden, "voc", axis=1, tiled=True),
        lax.all_gather(teacher_hidden, "voc", axis=1, tiled=True),
    )
    vocab_local = student_head.shape[1]
    row_count = student_block.shape[0] // lax.axis_size("hid")
    joined = lax.psum_scatter(
        jnp.concatenate(
            [
                jnp.dot(student_block, student_head, preferred_element_type=jnp.float32),
                jnp.dot(teacher_block, teacher_head, preferred_element_type=jnp.float32),
            ],
            axis=1,
        ),
        "hid",
        scatter_dimension=0,
        tiled=True,
    )
    student_logits = joined[:, :vocab_local]
    teacher_logits = joined[:, vocab_local:]
    weights = lax.dynamic_slice_in_dim(loss_weight, lax.axis_index("hid") * row_count, row_count)
    divergence, scaled_gap = divergence_terms(student_logits, teacher_logits, weights)
    token_total = loss_weight.shape[0] * lax.axis_size("tok")
    loss_total = lax.psum(jnp.sum(divergence), ("tok", "hid"))
    grad_terms = lax.dot_general(
        lax.all_gather(scaled_gap, "hid", axis=0, tiled=True),
        student_head,
        (((1,), (1,)), ((), ())),
        preferred_element_type=jnp.float32,
    )
    grad_hidden = lax.psum_scatter(grad_terms, "voc", scatter_dimension=1, tiled=True).astype(
        jnp.bfloat16
    )
    mean_loss = loss_total / token_total
    return (grad_hidden, mean_loss)


def solution(mesh):
    placed = (
        P("tok", ("hid", "voc")),
        P("tok", ("hid", "voc")),
        P("hid", "voc"),
        P("hid", "voc"),
        P("tok"),
    )
    n, nt = mesh.shape["voc"], mesh.shape["tok"]
    if n == 4 and nt == 4 and mesh.shape["hid"] == 2:
        body = functools.partial(fused_shards, n, nt)
    else:
        body = plain_shards
    return jax.shard_map(
        body,
        mesh=mesh,
        in_specs=placed,
        out_specs=(P("tok", ("hid", "voc")), P()),
        check_vma=False,
    )
```

```python
import functools

import jax
import jax.numpy as jnp
from jax import lax
from jax.experimental import pallas as pl
from jax.experimental.pallas import tpu as pltpu
from jax.sharding import PartitionSpec as P

MESH = pl.DeviceIdType.MESH
F32 = jnp.float32
BF16 = jnp.bfloat16
GROUPS = 2


def fused(n, nt, ng, x_hbm, y_hbm, w_hbm, sw_hbm, tw_hbm, out, loss_out,
          x_ref, y_ref, w_ref, wf, tw, tg, sp, spx, ssum, srr, tacc, tpx, stat, gap, wcol, lossb, lossr, lossx, acc,
          lc, wz_s, wz_r, wt_s, wt_r, th_s, th_r, px_s, px_r, tx_s, tx_r, rs_s, rs_r,
          st_s, st_r, gz_s, gz_r, gx_s, gx_r, ls_s, ls_r):
    z = lax.axis_index("voc")
    t = lax.axis_index("tok")
    h = lax.axis_index("hid")
    rows, ks = x_ref.shape
    kt = y_ref.shape[1]
    half = rows // 2
    q = half // ng
    quarter = ks // nt
    eighth = quarter // 2
    partner = {"hid": 1 - h}
    mine = pl.ds(pl.multiple_of(h * half, half), half)
    theirs = pl.ds(pl.multiple_of((1 - h) * half, half), half)
    nbr = (t + 1 - 2 * lax.rem(t, 2), lax.rem(t + 2, 4))
    diag = nt - 1 - t
    at_end = jnp.logical_or(z == 0, z == n - 1)
    inside = jnp.logical_not(at_end)
    side_in = jnp.where(z < n // 2, 1, 0)
    side_out = 1 - side_in
    step_in = 2 * side_in - 1
    near, mid, far = z + step_in, z + 2 * step_in, z + 3 * step_in
    inner, beyond, outer = z + step_in, z + 2 * step_in, z - step_in

    def rc(src, dst, ss, rs, dev):
        return pltpu.make_async_remote_copy(
            src_ref=src, dst_ref=dst, send_sem=ss, recv_sem=rs,
            device_id=dev, device_id_type=MESH)

    def zdev(k):
        return lax.rem(z + k, n)

    def group(c, g):
        return pl.ds(pl.multiple_of(c * half + g * q, q), q)

    own_w = pltpu.make_async_copy(sw_hbm.at[pl.ds(pl.multiple_of(z * ks, ks), ks)], wf.at[z], lc.at[n])
    own_w.start()
    ins = [pltpu.make_async_copy(a, b, lc.at[n + 1 + i])
           for i, (a, b) in enumerate(((x_hbm, x_ref), (y_hbm, y_ref), (w_hbm, w_ref)))]
    for c in ins:
        c.start()

    def tw_copy(i):
        return pltpu.make_async_copy(tw_hbm.at[pl.ds(pl.multiple_of(i * kt, kt), kt)], tw.at[i], lc.at[i])

    barrier = pltpu.get_barrier_semaphore()
    for k in range(1, n):
        pl.semaphore_signal(barrier, inc=1, device_id={"voc": zdev(k)}, device_id_type=MESH)
    for k in range(1, nt):
        pl.semaphore_signal(barrier, inc=1, device_id={"tok": lax.rem(t + k, nt)}, device_id_type=MESH)
    pl.semaphore_signal(barrier, inc=1, device_id=partner, device_id_type=MESH)
    pl.semaphore_wait(barrier, n - 1 + nt - 1 + 1)

    def part(i):
        return pl.ds(pl.multiple_of(i * quarter, quarter), quarter)

    def subpart(i, b):
        return pl.ds(pl.multiple_of(i * quarter + b * eighth, eighth), eighth)

    def wz(j):
        return rc(sw_hbm.at[pl.ds(pl.multiple_of(j * ks + t * quarter, quarter), quarter)],
                  wf.at[z, part(t)], wz_s.at[j], wz_r.at[z], {"voc": j})

    def wz_in(j):
        return rc(wf.at[j, part(t)], wf.at[j, part(t)], wz_s.at[j], wz_r.at[j], {"voc": j})

    def wt(j, k):
        return rc(wf.at[j, part(t)], wf.at[j, part(t)], wt_s.at[j, k], wt_r.at[j, k], {"tok": nbr[k]})

    def wt_in(j, k):
        return rc(wf.at[j, part(nbr[k])], wf.at[j, part(nbr[k])], wt_s.at[j, k], wt_r.at[j, k], {"tok": nbr[k]})

    def wd(j, k):
        piece = wf.at[j, subpart(nbr[k], k)]
        return rc(piece, piece, wt_s.at[j, 2 + k], wt_r.at[j, 2 + k], {"tok": nbr[1 - k]})

    def wd_in(j, k):
        piece = wf.at[j, subpart(diag, k)]
        return rc(piece, piece, wt_s.at[j, 2 + k], wt_r.at[j, 2 + k], {"tok": nbr[1 - k]})

    owner = (1 - h, h)

    def y_send(src, i, g, c, k, dev):
        rows_gc = group(owner[c], g)
        return rc(src.at[rows_gc], tg.at[i, rows_gc], th_s.at[k, 2 * g + c], th_r.at[i, 2 * g + c], {"voc": dev})

    def y_own(g, c, k, dev):
        return y_send(y_hbm, z, g, c, k, dev)

    def y_relay(i, g, c, k):
        return y_send(tg.at[i], i, g, c, k, outer)

    def y_out(g, k, dev, cs=(0, 1)):
        for c in cs:
            y_own(g, c, k, dev).start()

    @pl.when(at_end)
    def _():
        for j in (near, mid, far):
            wz(j).start()
        y_out(0, 0, near)

    @pl.when(inside)
    def _():
        for j in (outer, inner, beyond):
            wz(j).start()
        y_out(0, 1, outer)
        y_out(0, 0, inner)
        for g in range(1, ng):
            y_out(g, 1, outer)
            y_out(g, 0, inner)

    for k in range(n):
        tw_copy(zdev(k)).start()

    for c in ins:
        c.wait()
    wcol[...] = jnp.transpose(jnp.broadcast_to(w_ref[...], (rows, rows)))

    def w_arrive(j):
        wz_in(j).wait_recv()
        for k in range(2):
            wt(j, k).start()

    def w_spread(j):
        for k in range(2):
            wt_in(j, k).wait_recv()
            wd(j, k).start()

    def teacher_dot(src, i, g, first):
        step = kt // 2

        @pl.loop(0, 2)
        def _(s):
            cols = pl.ds(pl.multiple_of(s * step, step), step)
            both = jnp.concatenate([src[pl.ds(c * half + g * q, q), cols] for c in range(2)], axis=0)
            term = jnp.dot(both, tw[i, cols, :], preferred_element_type=F32)
            if first:
                @pl.when(s == 0)
                def _():
                    tacc[g] = term

                @pl.when(s > 0)
                def _():
                    tacc[g] += term
            else:
                tacc[g] += term

    def take_y(i, g, c, k=None):
        y_send(tg.at[i], i, g, c, 0, outer).wait_recv()
        if k is not None:
            y_relay(i, g, c, k).start()

    def dot_y(i, g):
        teacher_dot(tg.at[i], i, g, False)

    def split_y(i, g):
        step = kt // 2
        for c in range(2):
            take_y(i, g, c)
            mine_gc = pl.ds(pl.multiple_of(owner[c] * q, q), q)

            @pl.loop(0, 2)
            def _(s):
                cols = pl.ds(pl.multiple_of(s * step, step), step)
                term = jnp.dot(tg[i, group(owner[c], g), cols], tw[i, cols, :], preferred_element_type=F32)
                tacc[g, mine_gc, :] += term
            if c == 0:
                t_swap(g).start()

    def full_y(i, g, k=None):
        for c in range(2):
            take_y(i, g, c, k)
        dot_y(i, g)

    def student(j):
        sp[j] = jnp.dot(x_ref[...], wf[j], preferred_element_type=F32)
        rc(sp.at[j, theirs], spx.at[j], px_s.at[j], px_r.at[j], partner).start()

    def student_sum(j):
        rc(sp.at[j, theirs], spx.at[j], px_s.at[j], px_r.at[j], partner).wait_recv()
        ssum[j] = sp[j, mine, :] + spx[j]

    def rs(side, j):
        return rc(ssum.at[j], srr.at[side, j], rs_s.at[j], rs_r.at[side, j], {"voc": z + 2 * side - 1})

    def student_full(j):
        for k in range(2):
            wd_in(j, k).wait_recv()
        student(j)

    def rs_take(side, j):
        rs(side, j).wait_recv()
        ssum[j] += srr[side, j]

    def student_pass(j, side, upstream):
        student_sum(j)
        if upstream:
            rs_take(side, j)
        rs(side, j).start()

    def t_swap(g):
        return rc(tacc.at[g, pl.ds(pl.multiple_of((1 - h) * q, q), q)], tpx.at[g], tx_s.at[g], tx_r.at[g], partner)

    def stx(g, j, src):
        return rc(stat.at[g, src], stat.at[g, src], st_s.at[g, j], st_r.at[g, src], {"voc": j})

    def gz(g, j, src):
        return rc(gap.at[src, group(h, g)], gap.at[src, group(h, g)], gz_s.at[g, j], gz_r.at[g, src], {"voc": j})

    def gx(g, src, c):
        return rc(gap.at[src, group(c, g)], gap.at[src, group(c, g)], gx_s.at[g, src], gx_r.at[g, src], partner)

    def send_stats(g):
        t_swap(g).wait_recv()
        tl = tacc[g, pl.ds(pl.multiple_of(h * q, q), q), :] + tpx[g]
        tpx[g] = tl
        sl = ssum[z, pl.ds(g * q, q), :]
        ms = jnp.max(sl, axis=1, keepdims=True)
        ss = jnp.sum(jnp.exp(sl - ms), axis=1, keepdims=True)
        mt = jnp.max(tl, axis=1, keepdims=True)
        et = jnp.exp(tl - mt)
        st = jnp.sum(et, axis=1, keepdims=True)
        cr = jnp.sum(et * (tl - sl), axis=1, keepdims=True)
        lane = lax.broadcasted_iota(jnp.int32, (q, 128), 1)
        cols = jnp.where(lane == 0, ms, jnp.where(lane == 1, mt, jnp.where(
            lane == 2, ss, jnp.where(lane == 3, st, cr))))
        stat[g, z] = jnp.transpose(jnp.concatenate([cols] * (128 // q), axis=0))[:8]
        for k in (2, 1, 3):
            stx(g, zdev(k), z).start()

    def send_gap(g):
        for k in range(1, n):
            stx(g, zdev(k), zdev(k)).wait_recv()
        parts = [stat[g, j] for j in range(n)]
        top = parts[0]
        for p in parts[1:]:
            top = jnp.maximum(top, p)
        big_s, big_t = top[0:1], top[1:2]
        tot_s = jnp.zeros_like(big_s)
        tot_t = jnp.zeros_like(big_s)
        cross = jnp.zeros_like(big_s)
        for p in parts:
            es = jnp.exp(p[0:1] - big_s)
            ets = jnp.exp(p[1:2] - big_t)
            tot_s = tot_s + p[2:3] * es
            tot_t = tot_t + p[3:4] * ets
            cross = cross + p[4:5] * ets
        lse_s = big_s + jnp.log(tot_s)
        lse_t = big_t + jnp.log(tot_t)
        scale = wcol[group(h, g), :][:, 0:1]
        sub = lax.broadcasted_iota(jnp.int32, (128, 128), 0)
        back = jnp.transpose(jnp.where(sub == 0, lse_s, lse_t))[:q]
        col_s, col_t = back[:, 0:1], back[:, 1:2]
        sl = ssum[z, pl.ds(g * q, q), :]
        gap[z, group(h, g), :] = (scale * (jnp.exp(sl - col_s) - jnp.exp(tpx[g] - col_t))).astype(BF16)
        for k in (2, 1, 3):
            gz(g, zdev(k), z).start()
        gx(g, z, h).start()
        div = cross / tot_t - lse_t + lse_s
        first = lax.broadcasted_iota(jnp.int32, div.shape, 1) < q
        lossr[g] = jnp.broadcast_to(jnp.sum(jnp.where(first, div, 0.0), axis=1, keepdims=True), (8, 128))

    def take_gap(g, j):
        gz(g, j, j).wait_recv()
        gx(g, j, h).start()

    def grad_dot(g, j, first):
        gx(g, j, 1 - h).wait_recv()
        both = jnp.concatenate([gap[j, pl.ds(c * half + g * q, q), :] for c in range(2)], axis=0)
        term = lax.dot_general(both, wf[j], (((1,), (1,)), ((), ())), preferred_element_type=F32)
        if first:
            acc[g] = term
        else:
            acc[g] += term

    def store(g):
        for c in range(2):
            out[pl.ds(c * half + g * q, q), :] = acc[g, pl.ds(c * q, q), :].astype(BF16)

    def drain_bulk():
        for k in range(1, n):
            j = zdev(k)
            wz(j).wait_send()
            for b in range(2):
                wt(j, b).wait_send()
                wd(j, b).wait_send()
            rs(side_in, j).wait_send()
        for g in range(ng):
            for c in range(2):
                y_own(g, c, 0, near).wait_send()

                @pl.when(at_end)
                def _(g=g, c=c):
                    y_own(g, c, 1, mid).wait_send()

                @pl.when(inside)
                def _(g=g, c=c):
                    y_own(g, c, 1, outer).wait_send()
                    for k, j in ((2, beyond), (3, inner)):
                        y_relay(j, g, c, k).wait_send()
            t_swap(g).wait_send()
        for j in range(n):
            rc(sp.at[j, theirs], spx.at[j], px_s.at[j], px_r.at[j], partner).wait_send()

    def local_dots():
        for i in range(n):
            tw_copy(i).wait()
        for g in range(ng):
            teacher_dot(y_ref, z, g, True)
        own_w.wait()
        student(z)

    @pl.when(at_end)
    def _():
        w_arrive(near)
        local_dots()
        w_spread(near)
        student_full(near)
        w_arrive(far)
        w_spread(far)
        y_out(0, 1, mid)
        student_pass(near, side_in, False)
        w_arrive(mid)
        student_full(far)
        full_y(near, 0)
        student_pass(far, side_in, False)
        w_spread(mid)
        full_y(near, 1)
        student_full(mid)

        @pl.when(h == 1)
        def _():
            y_out(1, 1, mid)
        student_sum(z)
        student_pass(mid, side_in, False)

        @pl.when(h == 0)
        def _():
            y_out(1, 1, mid)
        y_out(1, 0, near)
        full_y(far, 0)
        full_y(mid, 0)
        t_swap(0).start()
        full_y(mid, 1)
        rs_take(side_out, z)
        send_stats(0)
        split_y(far, 1)

    @pl.when(inside)
    def _():
        w_arrive(outer)
        local_dots()
        w_spread(outer)
        w_arrive(inner)
        w_arrive(beyond)
        student_full(outer)
        w_spread(inner)
        w_spread(beyond)
        take_y(inner, 0, 0, 3)
        take_y(beyond, 0, 0, 2)
        student_full(inner)
        take_y(beyond, 0, 1, 2)
        dot_y(beyond, 0)
        full_y(outer, 0)
        take_y(inner, 0, 1, 3)
        student_full(beyond)
        student_pass(beyond, side_in, True)
        dot_y(inner, 0)
        t_swap(0).start()
        take_y(inner, 1, 0, 3)
        take_y(inner, 1, 1, 3)

        @pl.when(h == 1)
        def _():
            take_y(beyond, 1, 0, 2)
            take_y(beyond, 1, 1, 2)
            student_pass(outer, side_out, True)
            student_pass(inner, side_in, True)

        @pl.when(h == 0)
        def _():
            student_pass(outer, side_out, True)
            take_y(beyond, 1, 0, 2)
            student_pass(inner, side_in, True)
            take_y(beyond, 1, 1, 2)
        dot_y(inner, 1)
        dot_y(beyond, 1)
        student_sum(z)
        rs_take(side_in, z)
        rs_take(side_out, z)
        send_stats(0)
        split_y(outer, 1)

    def lp():
        return rc(lossb.at[0], lossb.at[1], ls_s.at[nt], ls_r.at[nt], partner)

    def ls(a, b):
        return rc(lossx.at[b], lossx.at[b], ls_s.at[a], ls_r.at[b], {"tok": a})

    send_stats(1)
    send_gap(0)
    drain_bulk()
    send_gap(1)
    lossb[0] = lossr[0] + lossr[1]
    lp().start()
    across = lax.rem(z + 2, n)
    order = (near, across, n * (n - 1) // 2 - z - near - across)
    grad_dot(0, z, True)
    for j in order:
        take_gap(0, j)
    lp().wait_recv()
    lossx[t] = lossb[0] + lossb[1]
    for k in range(1, nt):
        ls(lax.rem(t + k, nt), t).start()
    grad_dot(1, z, True)
    for j in order:
        grad_dot(0, j, False)
    store(0)
    for j in order:
        take_gap(1, j)
    for j in order:
        grad_dot(1, j, False)
    store(1)
    for k in range(1, nt):
        ls(t, lax.rem(t + k, nt)).wait_recv()
    total = lossx[0]
    for a in range(1, nt):
        total = total + lossx[a]
    loss_out[0, 0] = total[0, 0] / (rows * nt)

    for g in range(ng):
        for k in range(1, n):
            stx(g, zdev(k), z).wait_send()
            gz(g, zdev(k), z).wait_send()
        for j in range(n):
            gx(g, j, h).wait_send()
    lp().wait_send()
    for k in range(1, nt):
        ls(lax.rem(t + k, nt), t).wait_send()


def fused_shards(n, nt, student_hidden, teacher_hidden, student_head, teacher_head, loss_weight):
    rows, ks = student_hidden.shape
    kt = teacher_hidden.shape[1]
    v = student_head.shape[1]
    half = rows // 2
    ng = GROUPS
    q = half // ng
    dma = lambda *s: pltpu.SemaphoreType.DMA(s)
    vmem = lambda s, d: pltpu.VMEM(s, d)
    anywhere = pl.BlockSpec(memory_space=pl.ANY)
    grad, loss = pl.pallas_call(
        functools.partial(fused, n, nt, ng),
        out_shape=(pltpu.VMEM((rows, ks), BF16), pltpu.SMEM((1, 1), F32)),
        in_specs=[anywhere] * 5,
        out_specs=(pl.BlockSpec(memory_space=pltpu.VMEM), pl.BlockSpec(memory_space=pltpu.SMEM)),
        scratch_shapes=[
            vmem((rows, ks), BF16),
            vmem((rows, kt), BF16),
            vmem((1, rows), F32),
            vmem((n, ks, v), BF16),
            vmem((n, kt, v), BF16),
            vmem((n, rows, kt), BF16),
            vmem((n, rows, v), F32),
            vmem((n, half, v), F32),
            vmem((n, half, v), F32),
            vmem((2, n, half, v), F32),
            vmem((ng, 2 * q, v), F32),
            vmem((ng, q, v), F32),
            vmem((ng, n, 8, 128), F32),
            vmem((n, rows, v), BF16),
            vmem((rows, rows), F32),
            vmem((2, 8, 128), F32),
            vmem((ng, 8, 128), F32),
            vmem((nt, 8, 128), F32),
            vmem((ng, 2 * q, ks), F32),
            dma(n + 4),
            dma(n), dma(n), dma(n, 4), dma(n, 4),
            dma(4, 2 * ng), dma(n, 2 * ng),
            dma(n), dma(n), dma(ng), dma(ng), dma(n), dma(2, n),
            dma(ng, n), dma(ng, n), dma(ng, n), dma(ng, n), dma(ng, n), dma(ng, n),
            dma(nt + 1), dma(nt + 1),
        ],
        compiler_params=pltpu.CompilerParams(
            collective_id=0, has_side_effects=True, vmem_limit_bytes=60 << 20),
        name="divergence_grad",
    )(student_hidden, teacher_hidden, loss_weight.reshape(1, rows), student_head, teacher_head)
    return grad, loss.reshape(())


def divergence_terms(student_logits, teacher_logits, weights):
    differences = teacher_logits - student_logits
    peak_student, peak_teacher = lax.pmax(
        (jnp.max(student_logits, axis=1), jnp.max(teacher_logits, axis=1)), "voc"
    )
    scaled_student = jnp.exp(student_logits - peak_student[:, None])
    scaled_teacher = jnp.exp(teacher_logits - peak_teacher[:, None])
    total_student, total_teacher, cross_sum = lax.psum(
        (
            jnp.sum(scaled_student, axis=1),
            jnp.sum(scaled_teacher, axis=1),
            jnp.sum(scaled_teacher * differences, axis=1),
        ),
        "voc",
    )
    student_lse = peak_student + jnp.log(total_student)
    teacher_lse = peak_teacher + jnp.log(total_teacher)
    divergence = cross_sum / total_teacher - teacher_lse + student_lse
    prob_gap = jnp.exp(student_logits - student_lse[:, None]) - jnp.exp(
        teacher_logits - teacher_lse[:, None]
    )
    scaled_gap = (weights[:, None] * prob_gap).astype(jnp.bfloat16)
    return (divergence, scaled_gap)


def plain_shards(student_hidden, teacher_hidden, student_head, teacher_head, loss_weight):
    student_block, teacher_block = (
        lax.all_gather(student_hidden, "voc", axis=1, tiled=True),
        lax.all_gather(teacher_hidden, "voc", axis=1, tiled=True),
    )
    vocab_local = student_head.shape[1]
    row_count = student_block.shape[0] // lax.axis_size("hid")
    joined = lax.psum_scatter(
        jnp.concatenate(
            [
                jnp.dot(student_block, student_head, preferred_element_type=jnp.float32),
                jnp.dot(teacher_block, teacher_head, preferred_element_type=jnp.float32),
            ],
            axis=1,
        ),
        "hid",
        scatter_dimension=0,
        tiled=True,
    )
    student_logits = joined[:, :vocab_local]
    teacher_logits = joined[:, vocab_local:]
    weights = lax.dynamic_slice_in_dim(loss_weight, lax.axis_index("hid") * row_count, row_count)
    divergence, scaled_gap = divergence_terms(student_logits, teacher_logits, weights)
    token_total = loss_weight.shape[0] * lax.axis_size("tok")
    loss_total = lax.psum(jnp.sum(divergence), ("tok", "hid"))
    grad_terms = lax.dot_general(
        lax.all_gather(scaled_gap, "hid", axis=0, tiled=True),
        student_head,
        (((1,), (1,)), ((), ())),
        preferred_element_type=jnp.float32,
    )
    grad_hidden = lax.psum_scatter(grad_terms, "voc", scatter_dimension=1, tiled=True).astype(
        jnp.bfloat16
    )
    mean_loss = loss_total / token_total
    return (grad_hidden, mean_loss)


def solution(mesh):
    placed = (
        P("tok", ("hid", "voc")),
        P("tok", ("hid", "voc")),
        P("hid", "voc"),
        P("hid", "voc"),
        P("tok"),
    )
    n, nt = mesh.shape["voc"], mesh.shape["tok"]
    if n == 4 and nt == 4 and mesh.shape["hid"] == 2:
        body = functools.partial(fused_shards, n, nt)
    else:
        body = plain_shards
    return jax.shard_map(
        body,
        mesh=mesh,
        in_specs=placed,
        out_specs=(P("tok", ("hid", "voc")), P()),
        check_vma=False,
    )
```

```python
import functools

import jax
import jax.numpy as jnp
from jax import lax
from jax.experimental import pallas as pl
from jax.experimental.pallas import tpu as pltpu
from jax.sharding import PartitionSpec as P

MESH = pl.DeviceIdType.MESH
F32 = jnp.float32
BF16 = jnp.bfloat16
GROUPS = 2


def fused(n, nt, ng, x_hbm, y_hbm, w_hbm, sw_hbm, tw_hbm, out, loss_out,
          x_ref, y_ref, w_ref, wf, tw, tg, sp, spx, ssum, srr, tacc, tpx, stat, gap, wcol, lossb, lossr, lossx, acc,
          lc, wz_s, wz_r, wt_s, wt_r, th_s, th_r, px_s, px_r, tx_s, tx_r, rs_s, rs_r,
          st_s, st_r, gz_s, gz_r, gx_s, gx_r, ls_s, ls_r):
    z = lax.axis_index("voc")
    t = lax.axis_index("tok")
    h = lax.axis_index("hid")
    rows, ks = x_ref.shape
    kt = y_ref.shape[1]
    half = rows // 2
    q = half // ng
    quarter = ks // nt
    eighth = quarter // 2
    partner = {"hid": 1 - h}
    mine = pl.ds(pl.multiple_of(h * half, half), half)
    theirs = pl.ds(pl.multiple_of((1 - h) * half, half), half)
    nbr = (t + 1 - 2 * lax.rem(t, 2), lax.rem(t + 2, 4))
    diag = nt - 1 - t
    at_end = jnp.logical_or(z == 0, z == n - 1)
    inside = jnp.logical_not(at_end)
    side_in = jnp.where(z < n // 2, 1, 0)
    side_out = 1 - side_in
    step_in = 2 * side_in - 1
    near, mid, far = z + step_in, z + 2 * step_in, z + 3 * step_in
    inner, beyond, outer = z + step_in, z + 2 * step_in, z - step_in

    def rc(src, dst, ss, rs, dev):
        return pltpu.make_async_remote_copy(
            src_ref=src, dst_ref=dst, send_sem=ss, recv_sem=rs,
            device_id=dev, device_id_type=MESH)

    def zdev(k):
        return lax.rem(z + k, n)

    def group(c, g):
        return pl.ds(pl.multiple_of(c * half + g * q, q), q)

    own_w = pltpu.make_async_copy(sw_hbm.at[pl.ds(pl.multiple_of(z * ks, ks), ks)], wf.at[z], lc.at[n])
    own_w.start()
    ins = [pltpu.make_async_copy(a, b, lc.at[n + 1 + i])
           for i, (a, b) in enumerate(((x_hbm, x_ref), (y_hbm, y_ref), (w_hbm, w_ref)))]
    for c in ins:
        c.start()

    def tw_copy(i):
        return pltpu.make_async_copy(tw_hbm.at[pl.ds(pl.multiple_of(i * kt, kt), kt)], tw.at[i], lc.at[i])

    barrier = pltpu.get_barrier_semaphore()
    for k in range(1, n):
        pl.semaphore_signal(barrier, inc=1, device_id={"voc": zdev(k)}, device_id_type=MESH)
    for k in range(1, nt):
        pl.semaphore_signal(barrier, inc=1, device_id={"tok": lax.rem(t + k, nt)}, device_id_type=MESH)
    pl.semaphore_signal(barrier, inc=1, device_id=partner, device_id_type=MESH)
    pl.semaphore_wait(barrier, n - 1 + nt - 1 + 1)

    def part(i):
        return pl.ds(pl.multiple_of(i * quarter, quarter), quarter)

    def subpart(i, b):
        return pl.ds(pl.multiple_of(i * quarter + b * eighth, eighth), eighth)

    def wz(j):
        return rc(sw_hbm.at[pl.ds(pl.multiple_of(j * ks + t * quarter, quarter), quarter)],
                  wf.at[z, part(t)], wz_s.at[j], wz_r.at[z], {"voc": j})

    def wz_in(j):
        return rc(wf.at[j, part(t)], wf.at[j, part(t)], wz_s.at[j], wz_r.at[j], {"voc": j})

    def wt(j, k):
        return rc(wf.at[j, part(t)], wf.at[j, part(t)], wt_s.at[j, k], wt_r.at[j, k], {"tok": nbr[k]})

    def wt_in(j, k):
        return rc(wf.at[j, part(nbr[k])], wf.at[j, part(nbr[k])], wt_s.at[j, k], wt_r.at[j, k], {"tok": nbr[k]})

    def wd(j, k):
        piece = wf.at[j, subpart(nbr[k], k)]
        return rc(piece, piece, wt_s.at[j, 2 + k], wt_r.at[j, 2 + k], {"tok": nbr[1 - k]})

    def wd_in(j, k):
        piece = wf.at[j, subpart(diag, k)]
        return rc(piece, piece, wt_s.at[j, 2 + k], wt_r.at[j, 2 + k], {"tok": nbr[1 - k]})

    owner = (1 - h, h)

    def y_send(src, i, g, c, k, dev):
        rows_gc = group(owner[c], g)
        return rc(src.at[rows_gc], tg.at[i, rows_gc], th_s.at[k, 2 * g + c], th_r.at[i, 2 * g + c], {"voc": dev})

    def y_own(g, c, k, dev):
        return y_send(y_hbm, z, g, c, k, dev)

    def y_relay(i, g, c, k):
        return y_send(tg.at[i], i, g, c, k, outer)

    def y_out(g, k, dev, cs=(0, 1)):
        for c in cs:
            y_own(g, c, k, dev).start()

    @pl.when(at_end)
    def _():
        for j in (near, mid, far):
            wz(j).start()
        y_out(0, 0, near)

    @pl.when(inside)
    def _():
        for j in (outer, inner, beyond):
            wz(j).start()
        y_out(0, 1, outer)
        y_out(0, 0, inner)
        for g in range(1, ng):
            y_out(g, 1, outer)
            y_out(g, 0, inner)

    for k in range(n):
        tw_copy(zdev(k)).start()

    for c in ins:
        c.wait()
    wcol[...] = jnp.transpose(jnp.broadcast_to(w_ref[...], (rows, rows)))

    def w_arrive(j):
        wz_in(j).wait_recv()
        for k in range(2):
            wt(j, k).start()

    def w_spread(j):
        for k in range(2):
            wt_in(j, k).wait_recv()
            wd(j, k).start()

    def teacher_dot(src, i, g, first):
        step = kt // 2

        @pl.loop(0, 2)
        def _(s):
            cols = pl.ds(pl.multiple_of(s * step, step), step)
            both = jnp.concatenate([src[pl.ds(c * half + g * q, q), cols] for c in range(2)], axis=0)
            term = jnp.dot(both, tw[i, cols, :], preferred_element_type=F32)
            if first:
                @pl.when(s == 0)
                def _():
                    tacc[g] = term

                @pl.when(s > 0)
                def _():
                    tacc[g] += term
            else:
                tacc[g] += term

    def take_y(i, g, c, k=None):
        y_send(tg.at[i], i, g, c, 0, outer).wait_recv()
        if k is not None:
            y_relay(i, g, c, k).start()

    def dot_y(i, g):
        teacher_dot(tg.at[i], i, g, False)

    def split_y(i, g):
        for c in range(2):
            take_y(i, g, c)
            mine_gc = pl.ds(pl.multiple_of(owner[c] * q, q), q)
            tacc[g, mine_gc, :] += jnp.dot(tg[i, group(owner[c], g), :], tw[i], preferred_element_type=F32)
            if c == 0:
                t_swap(g).start()

    def full_y(i, g, k=None):
        for c in range(2):
            take_y(i, g, c, k)
        dot_y(i, g)

    def student(j):
        sp[j, theirs, :] = jnp.dot(x_ref[theirs, :], wf[j], preferred_element_type=F32)
        rc(sp.at[j, theirs], spx.at[j], px_s.at[j], px_r.at[j], partner).start()
        sp[j, mine, :] = jnp.dot(x_ref[mine, :], wf[j], preferred_element_type=F32)

    def student_sum(j):
        rc(sp.at[j, theirs], spx.at[j], px_s.at[j], px_r.at[j], partner).wait_recv()
        ssum[j] = sp[j, mine, :] + spx[j]

    def rs(side, j):
        return rc(ssum.at[j], srr.at[side, j], rs_s.at[j], rs_r.at[side, j], {"voc": z + 2 * side - 1})

    def student_full(j):
        for k in range(2):
            wd_in(j, k).wait_recv()
        student(j)

    def rs_take(side, j):
        rs(side, j).wait_recv()
        ssum[j] += srr[side, j]

    def student_pass(j, side, upstream):
        student_sum(j)
        if upstream:
            rs_take(side, j)
        rs(side, j).start()

    def t_swap(g):
        return rc(tacc.at[g, pl.ds(pl.multiple_of((1 - h) * q, q), q)], tpx.at[g], tx_s.at[g], tx_r.at[g], partner)

    def stx(g, j, src):
        return rc(stat.at[g, src], stat.at[g, src], st_s.at[g, j], st_r.at[g, src], {"voc": j})

    def gz(g, j, src):
        return rc(gap.at[src, group(h, g)], gap.at[src, group(h, g)], gz_s.at[g, j], gz_r.at[g, src], {"voc": j})

    def gx(g, src, c):
        return rc(gap.at[src, group(c, g)], gap.at[src, group(c, g)], gx_s.at[g, src], gx_r.at[g, src], partner)

    def send_stats(g):
        t_swap(g).wait_recv()
        tl = tacc[g, pl.ds(pl.multiple_of(h * q, q), q), :] + tpx[g]
        tpx[g] = tl
        sl = ssum[z, pl.ds(g * q, q), :]
        ms = jnp.max(sl, axis=1, keepdims=True)
        ss = jnp.sum(jnp.exp(sl - ms), axis=1, keepdims=True)
        mt = jnp.max(tl, axis=1, keepdims=True)
        et = jnp.exp(tl - mt)
        st = jnp.sum(et, axis=1, keepdims=True)
        cr = jnp.sum(et * (tl - sl), axis=1, keepdims=True)
        lane = lax.broadcasted_iota(jnp.int32, (q, 128), 1)
        cols = jnp.where(lane == 0, ms, jnp.where(lane == 1, mt, jnp.where(
            lane == 2, ss, jnp.where(lane == 3, st, cr))))
        stat[g, z] = jnp.transpose(jnp.concatenate([cols] * (128 // q), axis=0))[:8]
        for k in (2, 1, 3):
            stx(g, zdev(k), z).start()

    def send_gap(g):
        for k in range(1, n):
            stx(g, zdev(k), zdev(k)).wait_recv()
        parts = [stat[g, j] for j in range(n)]
        top = parts[0]
        for p in parts[1:]:
            top = jnp.maximum(top, p)
        big_s, big_t = top[0:1], top[1:2]
        tot_s = jnp.zeros_like(big_s)
        tot_t = jnp.zeros_like(big_s)
        cross = jnp.zeros_like(big_s)
        for p in parts:
            es = jnp.exp(p[0:1] - big_s)
            ets = jnp.exp(p[1:2] - big_t)
            tot_s = tot_s + p[2:3] * es
            tot_t = tot_t + p[3:4] * ets
            cross = cross + p[4:5] * ets
        lse_s = big_s + jnp.log(tot_s)
        lse_t = big_t + jnp.log(tot_t)
        scale = wcol[group(h, g), :][:, 0:1]
        sub = lax.broadcasted_iota(jnp.int32, (128, 128), 0)
        back = jnp.transpose(jnp.where(sub == 0, lse_s, lse_t))[:q]
        col_s, col_t = back[:, 0:1], back[:, 1:2]
        sl = ssum[z, pl.ds(g * q, q), :]
        gap[z, group(h, g), :] = (scale * (jnp.exp(sl - col_s) - jnp.exp(tpx[g] - col_t))).astype(BF16)
        for k in (2, 1, 3):
            gz(g, zdev(k), z).start()
        gx(g, z, h).start()
        div = cross / tot_t - lse_t + lse_s
        first = lax.broadcasted_iota(jnp.int32, div.shape, 1) < q
        lossr[g] = jnp.broadcast_to(jnp.sum(jnp.where(first, div, 0.0), axis=1, keepdims=True), (8, 128))

    def take_gap(g, j):
        gz(g, j, j).wait_recv()
        gx(g, j, h).start()

    def grad_dot(g, j, first):
        gx(g, j, 1 - h).wait_recv()
        both = jnp.concatenate([gap[j, pl.ds(c * half + g * q, q), :] for c in range(2)], axis=0)
        term = lax.dot_general(both, wf[j], (((1,), (1,)), ((), ())), preferred_element_type=F32)
        if first:
            acc[g] = term
        else:
            acc[g] += term

    def store(g):
        for c in range(2):
            out[pl.ds(c * half + g * q, q), :] = acc[g, pl.ds(c * q, q), :].astype(BF16)

    def drain_bulk():
        for k in range(1, n):
            j = zdev(k)
            wz(j).wait_send()
            for b in range(2):
                wt(j, b).wait_send()
                wd(j, b).wait_send()
            rs(side_in, j).wait_send()
        for g in range(ng):
            for c in range(2):
                y_own(g, c, 0, near).wait_send()

                @pl.when(at_end)
                def _(g=g, c=c):
                    y_own(g, c, 1, mid).wait_send()

                @pl.when(inside)
                def _(g=g, c=c):
                    y_own(g, c, 1, outer).wait_send()
                    for k, j in ((2, beyond), (3, inner)):
                        y_relay(j, g, c, k).wait_send()
            t_swap(g).wait_send()
        for j in range(n):
            rc(sp.at[j, theirs], spx.at[j], px_s.at[j], px_r.at[j], partner).wait_send()

    def local_dots():
        for i in range(n):
            tw_copy(i).wait()
        for g in range(ng):
            teacher_dot(y_ref, z, g, True)
        own_w.wait()
        student(z)

    @pl.when(at_end)
    def _():
        w_arrive(near)
        local_dots()
        w_spread(near)
        student_full(near)
        w_arrive(far)
        w_spread(far)
        y_out(0, 1, mid)
        student_pass(near, side_in, False)
        w_arrive(mid)
        student_full(far)
        full_y(near, 0)
        student_pass(far, side_in, False)
        w_spread(mid)
        full_y(near, 1)
        student_full(mid)

        @pl.when(h == 1)
        def _():
            y_out(1, 1, mid)
        student_sum(z)
        student_pass(mid, side_in, False)

        @pl.when(h == 0)
        def _():
            y_out(1, 1, mid)
        y_out(1, 0, near)
        full_y(far, 0)
        full_y(mid, 0)
        t_swap(0).start()
        full_y(mid, 1)
        rs_take(side_out, z)
        send_stats(0)
        split_y(far, 1)

    @pl.when(inside)
    def _():
        w_arrive(outer)
        local_dots()
        w_spread(outer)
        w_arrive(inner)
        w_arrive(beyond)
        student_full(outer)
        w_spread(inner)
        w_spread(beyond)
        take_y(inner, 0, 0, 3)
        take_y(beyond, 0, 0, 2)
        student_full(inner)
        take_y(beyond, 0, 1, 2)
        dot_y(beyond, 0)
        full_y(outer, 0)
        take_y(inner, 0, 1, 3)
        student_full(beyond)
        student_pass(beyond, side_in, True)
        dot_y(inner, 0)
        t_swap(0).start()
        take_y(inner, 1, 0, 3)
        take_y(inner, 1, 1, 3)

        @pl.when(h == 1)
        def _():
            take_y(beyond, 1, 0, 2)
            take_y(beyond, 1, 1, 2)
            student_pass(outer, side_out, True)
            student_pass(inner, side_in, True)

        @pl.when(h == 0)
        def _():
            student_pass(outer, side_out, True)
            take_y(beyond, 1, 0, 2)
            student_pass(inner, side_in, True)
            take_y(beyond, 1, 1, 2)
        dot_y(inner, 1)
        dot_y(beyond, 1)
        student_sum(z)
        rs_take(side_in, z)
        rs_take(side_out, z)
        send_stats(0)
        split_y(outer, 1)

    def lp():
        return rc(lossb.at[0], lossb.at[1], ls_s.at[nt], ls_r.at[nt], partner)

    def ls(a, b):
        return rc(lossx.at[b], lossx.at[b], ls_s.at[a], ls_r.at[b], {"tok": a})

    send_stats(1)
    send_gap(0)
    drain_bulk()
    send_gap(1)
    lossb[0] = lossr[0] + lossr[1]
    lp().start()
    across = lax.rem(z + 2, n)
    order = (near, across, n * (n - 1) // 2 - z - near - across)
    grad_dot(0, z, True)
    for j in order:
        take_gap(0, j)
    lp().wait_recv()
    lossx[t] = lossb[0] + lossb[1]
    for k in range(1, nt):
        ls(lax.rem(t + k, nt), t).start()
    grad_dot(1, z, True)
    for j in order:
        grad_dot(0, j, False)
    store(0)
    for j in order:
        take_gap(1, j)
    for j in order:
        grad_dot(1, j, False)
    store(1)
    for k in range(1, nt):
        ls(t, lax.rem(t + k, nt)).wait_recv()
    total = lossx[0]
    for a in range(1, nt):
        total = total + lossx[a]
    loss_out[0, 0] = total[0, 0] / (rows * nt)

    for g in range(ng):
        for k in range(1, n):
            stx(g, zdev(k), z).wait_send()
            gz(g, zdev(k), z).wait_send()
        for j in range(n):
            gx(g, j, h).wait_send()
    lp().wait_send()
    for k in range(1, nt):
        ls(lax.rem(t + k, nt), t).wait_send()


def fused_shards(n, nt, student_hidden, teacher_hidden, student_head, teacher_head, loss_weight):
    rows, ks = student_hidden.shape
    kt = teacher_hidden.shape[1]
    v = student_head.shape[1]
    half = rows // 2
    ng = GROUPS
    q = half // ng
    dma = lambda *s: pltpu.SemaphoreType.DMA(s)
    vmem = lambda s, d: pltpu.VMEM(s, d)
    anywhere = pl.BlockSpec(memory_space=pl.ANY)
    grad, loss = pl.pallas_call(
        functools.partial(fused, n, nt, ng),
        out_shape=(pltpu.VMEM((rows, ks), BF16), pltpu.SMEM((1, 1), F32)),
        in_specs=[anywhere] * 5,
        out_specs=(pl.BlockSpec(memory_space=pltpu.VMEM), pl.BlockSpec(memory_space=pltpu.SMEM)),
        scratch_shapes=[
            vmem((rows, ks), BF16),
            vmem((rows, kt), BF16),
            vmem((1, rows), F32),
            vmem((n, ks, v), BF16),
            vmem((n, kt, v), BF16),
            vmem((n, rows, kt), BF16),
            vmem((n, rows, v), F32),
            vmem((n, half, v), F32),
            vmem((n, half, v), F32),
            vmem((2, n, half, v), F32),
            vmem((ng, 2 * q, v), F32),
            vmem((ng, q, v), F32),
            vmem((ng, n, 8, 128), F32),
            vmem((n, rows, v), BF16),
            vmem((rows, rows), F32),
            vmem((2, 8, 128), F32),
            vmem((ng, 8, 128), F32),
            vmem((nt, 8, 128), F32),
            vmem((ng, 2 * q, ks), F32),
            dma(n + 4),
            dma(n), dma(n), dma(n, 4), dma(n, 4),
            dma(4, 2 * ng), dma(n, 2 * ng),
            dma(n), dma(n), dma(ng), dma(ng), dma(n), dma(2, n),
            dma(ng, n), dma(ng, n), dma(ng, n), dma(ng, n), dma(ng, n), dma(ng, n),
            dma(nt + 1), dma(nt + 1),
        ],
        compiler_params=pltpu.CompilerParams(
            collective_id=0, has_side_effects=True, vmem_limit_bytes=60 << 20),
        name="divergence_grad",
    )(student_hidden, teacher_hidden, loss_weight.reshape(1, rows), student_head, teacher_head)
    return grad, loss.reshape(())


def divergence_terms(student_logits, teacher_logits, weights):
    differences = teacher_logits - student_logits
    peak_student, peak_teacher = lax.pmax(
        (jnp.max(student_logits, axis=1), jnp.max(teacher_logits, axis=1)), "voc"
    )
    scaled_student = jnp.exp(student_logits - peak_student[:, None])
    scaled_teacher = jnp.exp(teacher_logits - peak_teacher[:, None])
    total_student, total_teacher, cross_sum = lax.psum(
        (
            jnp.sum(scaled_student, axis=1),
            jnp.sum(scaled_teacher, axis=1),
            jnp.sum(scaled_teacher * differences, axis=1),
        ),
        "voc",
    )
    student_lse = peak_student + jnp.log(total_student)
    teacher_lse = peak_teacher + jnp.log(total_teacher)
    divergence = cross_sum / total_teacher - teacher_lse + student_lse
    prob_gap = jnp.exp(student_logits - student_lse[:, None]) - jnp.exp(
        teacher_logits - teacher_lse[:, None]
    )
    scaled_gap = (weights[:, None] * prob_gap).astype(jnp.bfloat16)
    return (divergence, scaled_gap)


def plain_shards(student_hidden, teacher_hidden, student_head, teacher_head, loss_weight):
    student_block, teacher_block = (
        lax.all_gather(student_hidden, "voc", axis=1, tiled=True),
        lax.all_gather(teacher_hidden, "voc", axis=1, tiled=True),
    )
    vocab_local = student_head.shape[1]
    row_count = student_block.shape[0] // lax.axis_size("hid")
    joined = lax.psum_scatter(
        jnp.concatenate(
            [
                jnp.dot(student_block, student_head, preferred_element_type=jnp.float32),
                jnp.dot(teacher_block, teacher_head, preferred_element_type=jnp.float32),
            ],
            axis=1,
        ),
        "hid",
        scatter_dimension=0,
        tiled=True,
    )
    student_logits = joined[:, :vocab_local]
    teacher_logits = joined[:, vocab_local:]
    weights = lax.dynamic_slice_in_dim(loss_weight, lax.axis_index("hid") * row_count, row_count)
    divergence, scaled_gap = divergence_terms(student_logits, teacher_logits, weights)
    token_total = loss_weight.shape[0] * lax.axis_size("tok")
    loss_total = lax.psum(jnp.sum(divergence), ("tok", "hid"))
    grad_terms = lax.dot_general(
        lax.all_gather(scaled_gap, "hid", axis=0, tiled=True),
        student_head,
        (((1,), (1,)), ((), ())),
        preferred_element_type=jnp.float32,
    )
    grad_hidden = lax.psum_scatter(grad_terms, "voc", scatter_dimension=1, tiled=True).astype(
        jnp.bfloat16
    )
    mean_loss = loss_total / token_total
    return (grad_hidden, mean_loss)


def solution(mesh):
    placed = (
        P("tok", ("hid", "voc")),
        P("tok", ("hid", "voc")),
        P("hid", "voc"),
        P("hid", "voc"),
        P("tok"),
    )
    n, nt = mesh.shape["voc"], mesh.shape["tok"]
    if n == 4 and nt == 4 and mesh.shape["hid"] == 2:
        body = functools.partial(fused_shards, n, nt)
    else:
        body = plain_shards
    return jax.shard_map(
        body,
        mesh=mesh,
        in_specs=placed,
        out_specs=(P("tok", ("hid", "voc")), P()),
        check_vma=False,
    )
```
